32 devices in a mesh: aux: 16 (over z, x, core), pair: 2 (over y).
Axes of the slice: x: 2, y: 2, z: 4, core: 2. Of those that a mesh axis runs over, the one named last changes fastest.
Arguments:
- three_center: bfloat16 [128, 64, 1024], P('aux', 'pair'), may hold values from -6 to 6
- tile_live: int32 [16, 64], P('aux', 'pair'), may hold values from 0 to 1
- pair_atoms: int32 [64], replicated, may hold values from 0 to 63, each once
- green_occ: bfloat16 [256, 256], replicated, may hold values from -0.375 to 0.375
- green_vir: bfloat16 [256, 256], replicated, may hold values from -0.375 to 0.375
- screened: bfloat16 [128, 40], P('aux'), may hold values from -1 to 1
Outputs:
- polarizability: float32 [128, 40], P('aux', 'pair')
- self_energy: float32 [64, 1024], P('pair')
The draws below stay inside these ranges and needn't reach their ends.
Inputs may be any that keep to these rules, and one draw needn't show every extreme that they name: `pair_atoms`: a permutation of the 64 atom pairs.
All inputs are finite; a program needn't handle non-finite values.
Results may differ from the reference program's by a relative error of at most 0.0043.
Values may be sent and summed in bfloat16 or wider, within the bound.
No kernel may reach another device: no remote copies, remote signals or barrier semaphores. Data moves between devices by JAX's collectives and lax.ppermute only.
A program may use at most 64 MiB of HBM per device.

```python
import jax
import jax.numpy as jnp
from jax import lax

OA = 32
NAT = 8
AUX_DEV = 8
REACH = 2
NORB = 256
PAIR = 1024
NPT = 64
AUX_BLOCKS = 16
NAUX = 128
WIN = 40


def draw_tile_live(key, part):
    key_rows = jax.random.fold_in(key, 11)
    key_cells = jax.random.fold_in(key, 23)
    level = jax.random.randint(key_rows, (AUX_BLOCKS, 1), 1, 5)
    cells = jax.random.randint(key_cells, (AUX_BLOCKS, NPT), 0, 4)
    return (cells < level).astype(jnp.int32)


def shard_levels(own_key, dims, pieces, low, largest):
    def one(position, blocks):
        heights = jax.random.uniform(jax.random.fold_in(jax.random.fold_in(own_key, 6), position), (blocks,), jnp.float32, low / len(pieces), largest / len(pieces))
        return jnp.repeat(jnp.exp(heights), dims[position] // blocks).reshape((-1,) + (1,) * (len(dims) - position - 1))

    factor_of = one(*pieces[0])
    for cut in pieces[1:]:
        factor_of = factor_of * one(*cut)
    return factor_of


def centred(own_key, shape, scale, limit, split=(), kind=jnp.bfloat16):
    entries = jax.random.normal(own_key, shape, jnp.float32) * scale
    if len(split) > 0:
        entries = shard_levels(own_key, shape, split, -0.22, 0.18) * entries
    return jnp.clip(entries, min=-limit, max=limit).astype(kind)


def setup_inputs(seed: int = 0) -> dict:
    key_of = jax.random.split(jax.random.key(seed), 7)
    return {
        "three_center": centred(key_of[0], (NAUX, NPT, PAIR), 1.0, 6.0, ((0, 16), (1, 2))),
        "tile_live": draw_tile_live(jax.random.fold_in(key_of[6], 71), 0),
        "pair_atoms": jax.random.permutation(key_of[2], NPT).astype(jnp.int32),
        "green_occ": centred(key_of[3], (NORB, NORB), NORB ** -0.5, 0.375),
        "green_vir": centred(key_of[4], (NORB, NORB), NORB ** -0.5, 0.375),
        "screened": centred(key_of[5], (NAUX, WIN), WIN ** -0.5, 1.0, ((0, 16),)),
    }


def rounded(values):
    return lax.optimization_barrier(values.astype(jnp.bfloat16)).astype(jnp.float32)


def tiles_to_matrix(tile_data, inverse):
    tile_rows = tile_data.shape[0]
    ordered = jnp.take(tile_data, inverse, axis=1)
    reshaped = ordered.reshape(tile_rows, NAT, NAT, OA, OA)
    return jnp.transpose(reshaped, (0, 1, 3, 2, 4)).reshape(tile_rows, NAT * OA, NAT * OA)


def matrix_to_tiles(matrix, pair_atoms):
    tile_rows = matrix.shape[0]
    reshaped = matrix.reshape(tile_rows, NAT, OA, NAT, OA)
    ordered = jnp.transpose(reshaped, (0, 1, 3, 2, 4)).reshape(tile_rows, NAT * NAT, OA * OA)
    return jnp.take(ordered, pair_atoms, axis=1)


def reference(three_center, tile_live, pair_atoms, green_occ, green_vir, screened):
    aux_total = three_center.shape[0]
    block_count = aux_total // AUX_DEV
    live_rows = jnp.repeat(tile_live, AUX_DEV, axis=0).astype(jnp.bfloat16)
    masked = three_center * live_rows[:, :, None]
    inverse = jnp.argsort(pair_atoms).astype(jnp.int32)
    first_atom = pair_atoms // NAT
    second_atom = pair_atoms % NAT
    margin_rows = REACH * AUX_DEV
    padded = jnp.pad(masked, ((margin_rows, margin_rows), (0, 0), (0, 0)))
    occ_full = green_occ.astype(jnp.float32)
    vir_full = green_vir.astype(jnp.float32)
    chi_scale = 1.0 / (OA * NAT)
    sigma_scale = 1.0 / (aux_total * NAT * OA * NAT) ** 0.5

    def one_block(block_index):
        row_start = block_index * AUX_DEV
        own_rows = lax.dynamic_slice_in_dim(masked, row_start, AUX_DEV, 0)
        window = lax.dynamic_slice_in_dim(padded, row_start, WIN, 0)
        orbital_form = tiles_to_matrix(own_rows, inverse).astype(jnp.float32)
        left_half = rounded(jnp.einsum("lu,plm->pum", occ_full, orbital_form))
        full_form = rounded(jnp.einsum("pum,mv->puv", left_half, vir_full))
        products = matrix_to_tiles(full_form, pair_atoms)
        window_float = window.astype(jnp.float32)
        chi_block = jnp.einsum("pke,qke->pq", products, window_float) * chi_scale
        coupling = lax.dynamic_slice_in_dim(screened, row_start, AUX_DEV, 0).astype(jnp.float32)
        mixed_tiles = jnp.einsum("qw,wke->qke", coupling, window_float).astype(jnp.bfloat16)
        return chi_block, mixed_tiles

    chi_blocks, mixed_blocks = lax.map(one_block, jnp.arange(block_count, dtype=jnp.int32))
    polarizability = chi_blocks.reshape(aux_total, WIN)
    mixed_all = mixed_blocks.reshape(aux_total, NPT, OA * OA)
    occ_rows = jnp.take(occ_full.reshape(NAT, OA, NAT * OA), second_atom, axis=0)

    def accumulate(running, block_index):
        row_start = block_index * AUX_DEV
        own_rows = lax.dynamic_slice_in_dim(masked, row_start, AUX_DEV, 0)
        orbital_form = tiles_to_matrix(own_rows, inverse).astype(jnp.float32)
        mixed_tiles = lax.dynamic_slice_in_dim(mixed_all, row_start, AUX_DEV, 0).astype(jnp.float32)
        mixed_tiles = mixed_tiles.reshape(AUX_DEV, NPT, OA, OA)
        scaled_rows = rounded(jnp.einsum("qkml,kls->qkms", mixed_tiles, occ_rows))
        return running + jnp.einsum("qkms,qsn->kmn", scaled_rows, orbital_form), None

    start_sum = jnp.zeros((NPT, OA, NAT * OA), jnp.float32)
    term_sums, unused = lax.scan(accumulate, start_sum, jnp.arange(block_count, dtype=jnp.int32))
    atom_onehot = (first_atom[:, None] == jnp.arange(NAT, dtype=jnp.int32)[None, :]).astype(jnp.float32)
    by_atom = jnp.einsum("ka,kmn->amn", atom_onehot, term_sums, precision=lax.Precision.HIGHEST)
    self_energy = matrix_to_tiles(by_atom.reshape(1, NAT * OA, NAT * OA), pair_atoms)[0] * (-sigma_scale)
    return polarizability, self_energy
```

```python
import math

import jax
import jax.numpy as jnp
from jax import lax
from jax.experimental import pallas as pl
from jax.experimental.pallas import tpu as pltpu
from jax.sharding import PartitionSpec as P

OA = 32
NAT = 8
REACH = 2
BLK = 8
NORB = OA * NAT
PAIR = OA * OA
LANE = 128
RQ = LANE // OA
NQ = OA // RQ
LIVE_AT = 64
BF = jnp.bfloat16
F4 = jnp.float32


def iota(shape, dim):
    return lax.broadcasted_iota(jnp.int32, shape, dim)


def mm(a, b):
    return lax.dot_general(a, b, (((1,), (0,)), ((), ())), preferred_element_type=F4)


def mm_nt(a, b):
    return lax.dot_general(a, b, (((1,), (1,)), ((), ())), preferred_element_type=F4)


def mm_tn(a, b):
    return lax.dot_general(a, b, (((0,), (0,)), ((), ())), preferred_element_type=F4)


def onehot(cond):
    return cond.astype(F4).astype(BF)


def div(x, n):
    if n & (n - 1) == 0:
        return lax.shift_right_logical(x, jnp.full_like(x, n.bit_length() - 1))
    return x // n


def mod(x, n):
    if n & (n - 1) == 0:
        return x & (n - 1)
    return x % n


def mm_split(a, b):
    count = a.shape[0]
    high = a.astype(BF)
    rest = a - high.astype(F4)
    middle = rest.astype(BF)
    low = (rest - middle.astype(F4)).astype(BF)
    out = mm(jnp.concatenate([high.astype(F4), middle.astype(F4), low.astype(F4)], axis=0).astype(BF), b)
    return out[:count] + out[count : 2 * count] + out[2 * count :]


def pick_rows(count):
    return -(-count // LANE) * BLK


def slot_onehot(pair_row):
    count = pair_row.shape[1]
    slot = iota((NAT * NAT, count), 0)
    second = mod(div(slot, NAT), 2) * RQ + div(slot, 2 * NAT)
    return mod(slot, NAT) * NAT + second == pair_row


def to_matrix(tiles, swap):
    rows = [
        jnp.concatenate(
            [tiles[i * 2 * NAT : (i + 1) * 2 * NAT, q * LANE : (q + 1) * LANE] for i in range(RQ)],
            axis=1,
        )
        for q in range(NQ)
    ]
    mixed = mm(jnp.concatenate(rows, axis=0), swap)
    out = [
        jnp.concatenate(
            [
                mixed[(q * 2 + g) * NAT : (q * 2 + g + 1) * NAT, i * LANE : (i + 1) * LANE]
                for g in range(2)
            ],
            axis=1,
        )
        for i in range(RQ)
        for q in range(NQ)
    ]
    return jnp.concatenate(out, axis=0).astype(BF)


def from_matrix(matrix, swap):
    rows = [
        jnp.concatenate(
            [
                matrix[(i * NQ + q) * NAT : (i * NQ + q + 1) * NAT, g * LANE : (g + 1) * LANE]
                for i in range(RQ)
            ],
            axis=1,
        )
        for q in range(NQ)
        for g in range(2)
    ]
    mixed = mm(jnp.concatenate(rows, axis=0).astype(BF), swap).astype(BF)
    out = [
        jnp.concatenate(
            [
                mixed[q * 2 * NAT : (q + 1) * 2 * NAT, i * LANE : (i + 1) * LANE]
                for q in range(NQ)
            ],
            axis=1,
        )
        for i in range(RQ)
    ]
    return jnp.concatenate(out, axis=0)


def tables_kernel(occ_ref, vir_ref, swap_ref, both_ref, both_t_ref, cols_ref, vir_t_ref):
    size = RQ * LANE
    row = iota((size, size), 0)
    col = iota((size, size), 1)
    swapped = mod(div(row, OA), RQ) * LANE + div(row, LANE) * OA + mod(row, OA)
    swap_ref[...] = onehot(swapped == col)
    row = iota((NORB, NORB), 0)
    col = iota((NORB, NORB), 1)
    natural = mod(row, NAT) * OA + mod(div(row, NAT), NQ) * RQ + div(row, NAT * NQ)
    order = onehot(natural == col)
    occ = occ_ref[...]
    cols = mm_nt(occ, order).astype(BF)
    both = mm(order, cols)
    cols_ref[...] = cols
    both_ref[...] = both.astype(BF)
    both_t_ref[...] = both.T.astype(BF)
    vir_t_ref[...] = vir_ref[...].astype(F4).T.astype(BF)


def own_kernel(count, *refs):
    pairs_ref, metas = refs[0], refs[1 : 1 + count]
    pieces = refs[1 + count : 1 + 2 * count]
    swap_ref, both_ref, both_t_ref, cols_ref, vir_ref, vir_t_ref = refs[1 + 2 * count : 7 + 2 * count]
    matrix_ref, right_ref, z_ref, y_ref = refs[7 + 2 * count :]
    own_count = pieces[0].shape[1]
    swap = swap_ref[...]
    tiles = None
    for s in range(count):
        live = metas[s][0:1, LIVE_AT : LIVE_AT + own_count].astype(F4)
        select = (slot_onehot(pairs_ref[s : s + 1, :]).astype(F4) * live).astype(BF)
        part = mm(select, pieces[s][0])
        tiles = part if tiles is None else tiles + part
    own_select = onehot(slot_onehot(pairs_ref[0:1, :]))
    matrix = to_matrix(tiles.astype(BF), swap)
    matrix_ref[0] = matrix
    right_ref[0] = mm(matrix, cols_ref[...]).astype(BF)
    left = mm(both_t_ref[...], matrix).astype(BF)
    z_tiles = from_matrix(mm(left, vir_ref[...]), swap)
    z_ref[0] = mm_tn(own_select, z_tiles).astype(BF)
    left = mm(both_ref[...], matrix).astype(BF)
    y_tiles = from_matrix(mm(left, vir_t_ref[...]), swap)
    y_ref[0] = mm_tn(own_select, y_tiles).astype(BF)


def window_kernel(lanes, sigma_scale, chi_scale, place_ref, *refs):
    (pairs_ref, meta0, meta1, meta2, tile0, tile1a, tile1b, tile2) = refs[:8]
    (z_ref, y_ref, matrix_ref, right_ref, swap_ref, cols_ref, keep_ref, send_ref) = refs[8:]
    pair_count, own_count = pairs_ref.shape
    rows = BLK * own_count
    block, pair_at = place_ref[0], place_ref[1]
    row = iota((rows, rows), 0)
    col = iota((rows, rows), 1)
    same = (mod(row, own_count) == mod(col, own_count)).astype(F4)
    spread_row, spread_col = iota((LANE, rows), 0), iota((LANE, rows), 1)
    spread = onehot(spread_row == LIVE_AT + mod(spread_col, own_count))
    metas = [m[...] for m in (meta0, meta1, meta2)]
    masks = [same * mm(m, spread)[0:1, :] for m in metas]
    tiles = [tile0[...], tile1a[...] + tile1b[...], tile2[...]]
    expand = onehot(div(iota((rows, BLK), 0), own_count) == iota((rows, BLK), 1))
    own_weights = mm(expand, metas[0]).astype(BF)
    mixed = jnp.zeros((rows, PAIR), F4)
    for t in range(REACH + 1):
        pick = onehot(spread_row == (REACH + t) * BLK + div(spread_col, own_count))
        mixed = mixed + mm((mm(own_weights, pick) * masks[t]).astype(BF), tiles[t])
    other = jnp.zeros((rows, PAIR), F4)
    unspread = onehot(iota((BLK, rows), 0) == div(iota((BLK, rows), 1), own_count))
    for t in range(1, REACH + 1):
        pick = onehot(
            iota((rows, LANE), 1) == (REACH - t) * BLK + div(iota((rows, LANE), 0), own_count)
        )
        weights = mm(mm_nt(pick, metas[t]).astype(BF), unspread)
        other = other + mm((weights * masks[t]).astype(BF), tiles[t])
    mixed = mixed.astype(BF)
    other = other.astype(BF)
    swap = swap_ref[...]
    own_select = onehot(slot_onehot(pairs_ref[0:1, :]))
    total = jnp.zeros((NORB, NORB), F4)
    for r in range(BLK):
        at = slice(r * own_count, (r + 1) * own_count)
        value = to_matrix(mm(own_select, mixed[at]).astype(BF), swap)
        scaled = mm(value, cols_ref[...]).astype(BF)
        total = total + mm(scaled, matrix_ref[r])
        value = to_matrix(mm(own_select, other[at]).astype(BF), swap)
        total = total + mm(right_ref[r], value)
    total = total * -sigma_scale
    high = total.astype(BF).astype(F4)
    parts = [from_matrix(high, swap), from_matrix(total - high, swap)]
    parity = block & 1
    half = own_count // 2
    for s in range(pair_count):
        select = onehot(slot_onehot(pairs_ref[s : s + 1, :]))
        owned = mm_tn(select, parts[0]) + mm_tn(select, parts[1])
        first, second = owned[:half], owned[half:]
        keep = jnp.where(parity == 0, first, second)
        send = jnp.where(parity == 0, second, first)
        for q in range(NQ):
            keep_ref[s, q * half : (q + 1) * half, :] = keep[:, q * LANE : (q + 1) * LANE]
            send_ref[s, q * half : (q + 1) * half, :] = send[:, q * LANE : (q + 1) * LANE]

    chi = jnp.zeros((BLK, LANE), F4)
    for t in range(-REACH, REACH + 1):
        w = abs(t)
        if t < 0:
            cross = mm_nt(tiles[w], y_ref[...])
        else:
            cross = mm_nt(z_ref[...], tiles[w])
        cross = cross * masks[w]
        sums = jnp.concatenate(
            [
                jnp.sum(cross[p * own_count : (p + 1) * own_count], axis=0, keepdims=True)
                for p in range(BLK)
            ],
            axis=0,
        )
        pick = onehot(
            iota((rows, LANE), 1) == (REACH + t) * BLK + div(iota((rows, LANE), 0), own_count)
        )
        chi = chi + mm_split(sums, pick)
    chi = chi * chi_scale
    share = (2 * REACH + 1) * BLK // pair_count
    column = iota((LANE, 1), 0)
    target = block + jnp.maximum(REACH - div(column, BLK), 0)
    at_pair = jnp.zeros((LANE, 1), jnp.int32)
    for s in range(1, pair_count):
        at_pair = at_pair + (column >= s * share).astype(jnp.int32)
    place = mod(at_pair - pair_at + pair_count, pair_count) + (
        ((target ^ block) & 1) * pair_count
    )
    spot = place * lanes + div(target, 2) * share + column - at_pair * share
    spread = onehot(iota((LANE, 2 * pair_count * lanes), 1) == spot)
    placed = mm_split(chi, spread)
    for s in range(pair_count):
        for i in range(lanes // LANE):
            at = slice(NQ * half + i * BLK, NQ * half + (i + 1) * BLK)
            begin = s * lanes + i * LANE
            keep_ref[s, at, :] = placed[:, begin : begin + LANE]
            begin += pair_count * lanes
            send_ref[s, at, :] = placed[:, begin : begin + LANE]


def last_kernel(place_ref, own_ref, other_ref, chi_ref, energy_ref):
    half = energy_ref.shape[0] // 2
    share = chi_ref.shape[1]
    parity = place_ref[0] & 1
    own, other = own_ref[...], other_ref[...]
    first = jnp.where(parity == 0, own, other)
    second = jnp.where(parity == 0, other, own)
    for q in range(NQ):
        at = slice(q * LANE, (q + 1) * LANE)
        energy_ref[:half, at] = first[q * half : (q + 1) * half]
        energy_ref[half:, at] = second[q * half : (q + 1) * half]
    start = (place_ref[0] >> 1) * share
    total = None
    for i in range((own.shape[0] - NQ * half) // BLK):
        chi = own[NQ * half + i * BLK : NQ * half + (i + 1) * BLK]
        pick = onehot(iota((LANE, LANE), 0) + i * LANE == start + iota((LANE, LANE), 1))
        part = mm_split(chi, pick)
        total = part if total is None else total + part
    chi_ref[...] = total[:, :share]


def call(body, outs, *args, grid=None, in_specs=None, out_specs=None, flops=10**8):
    extra = {}
    if grid is not None:
        extra = dict(grid=grid, in_specs=in_specs, out_specs=out_specs)
    else:
        full = pl.BlockSpec(memory_space=pltpu.VMEM)
        extra = dict(
            in_specs=[
                pl.BlockSpec(memory_space=pltpu.SMEM) if a.ndim == 1 else full for a in args
            ],
            out_specs=jax.tree.map(lambda o: full, outs),
        )
    return pl.pallas_call(
        body,
        out_shape=outs,
        cost_estimate=pl.CostEstimate(flops=flops, bytes_accessed=10**6, transcendentals=0),
        **extra,
    )(*args)


def per_device(three_center, tile_live, pair_atoms, green_occ, green_vir, screened):
    block_rows, own_count = three_center.shape[:2]
    aux_count, pair_count = lax.axis_size("aux"), lax.axis_size("pair")
    block, pair_at = lax.axis_index("aux"), lax.axis_index("pair")
    rows = block_rows * own_count
    window = screened.shape[1]
    shape = jax.ShapeDtypeStruct

    def shifted(value, steps, parity=None):
        return lax.ppermute(
            value,
            "aux",
            [
                (s, s + steps)
                for s in range(aux_count)
                if 0 <= s + steps < aux_count and parity in (None, s % 2)
            ],
        )

    def turned(value, steps):
        return lax.ppermute(
            value, "pair", [(s, (s - steps) % pair_count) for s in range(pair_count)]
        )

    def flipped(value, mask):
        return lax.ppermute(value, "aux", [(s, s ^ mask) for s in range(aux_count)])

    live = jnp.broadcast_to(tile_live.astype(BF), (block_rows, own_count))
    meta = jnp.concatenate(
        [
            screened,
            jnp.zeros((block_rows, LIVE_AT - window), BF),
            live,
            jnp.zeros((block_rows, LANE - LIVE_AT - own_count), BF),
        ],
        axis=1,
    )
    far = shifted(three_center, -2)
    pieces = [three_center] + [turned(three_center, s) for s in range(1, pair_count)]
    near_even = shifted(three_center, -1, 1)
    metas = [meta] + [turned(meta, s) for s in range(1, pair_count)]
    meta_near, meta_far = shifted(meta, -1), shifted(meta, -2)
    near_odd = shifted(far, 1, 0)
    pairs = lax.dynamic_slice_in_dim(
        jnp.concatenate([pair_atoms, pair_atoms]), pair_at * own_count, pair_count * own_count
    ).reshape(pair_count, own_count)
    place = jnp.stack([block, pair_at]).astype(jnp.int32)

    square = shape((NORB, NORB), BF)
    swap, both, both_t, cols, vir_t = call(
        tables_kernel,
        [shape((RQ * LANE, RQ * LANE), BF), square, square, square, square],
        green_occ,
        green_vir,
    )

    def whole(value):
        return pl.BlockSpec(value.shape, lambda p: (0,) * value.ndim)

    def one(a, b):
        return pl.BlockSpec((1, a, b), lambda p: (p, 0, 0))

    fixed = [swap, both, both_t, cols, green_vir, vir_t]
    matrix, right, z, y = call(
        lambda *refs: own_kernel(pair_count, *refs),
        [
            shape((block_rows, NORB, NORB), BF),
            shape((block_rows, NORB, NORB), BF),
            shape((block_rows, own_count, PAIR), BF),
            shape((block_rows, own_count, PAIR), BF),
        ],
        pairs,
        *metas,
        *pieces,
        *fixed,
        grid=(block_rows,),
        in_specs=[whole(pairs)]
        + [whole(m) for m in metas]
        + [one(own_count, PAIR) for _ in pieces]
        + [whole(f) for f in fixed],
        out_specs=[one(NORB, NORB), one(NORB, NORB), one(own_count, PAIR), one(own_count, PAIR)],
    )

    lanes = -(-(aux_count // 2) * (window // pair_count) // LANE) * LANE
    message = shape((pair_count, own_count // 2 * NQ + lanes // LANE * BLK, LANE), F4)
    aux_total = block_rows * aux_count
    keep, send = call(
        lambda *refs: window_kernel(
            lanes, 1.0 / math.sqrt(aux_total * NAT * OA * NAT), 1.0 / (OA * NAT), *refs
        ),
        [message, message],
        place,
        pairs,
        meta,
        meta_near,
        meta_far,
        three_center.reshape(rows, PAIR),
        near_even.reshape(rows, PAIR),
        near_odd.reshape(rows, PAIR),
        far.reshape(rows, PAIR),
        z.reshape(rows, PAIR),
        y.reshape(rows, PAIR),
        matrix,
        right,
        swap,
        cols,
    )
    total = keep + flipped(send, 1)
    owned = total[0]
    for s in range(1, pair_count):
        owned = owned + turned(total[s], -s)
    mask = 2
    while mask < aux_count:
        owned = owned + flipped(owned, mask)
        mask *= 2
    polarizability, self_energy = call(
        last_kernel,
        [
            shape((block_rows, window // pair_count), F4),
            shape((own_count, PAIR), F4),
        ],
        place,
        owned,
        flipped(owned, 1),
    )
    return polarizability, self_energy


def solution(mesh):
    placed = (P("aux", "pair", None), P("aux", "pair"), P(), P(), P(), P("aux", None))
    return jax.shard_map(
        per_device,
        mesh=mesh,
        in_specs=placed,
        out_specs=(P("aux", "pair"), P("pair", None)),
        check_vma=False,
    )
```

```python
import math

import jax
import jax.numpy as jnp
from jax import lax
from jax.experimental import pallas as pl
from jax.experimental.pallas import tpu as pltpu
from jax.sharding import PartitionSpec as P


OA = 32
NAT = 8
REACH = 2
BLK = 8
NORB = OA * NAT
PAIR = OA * OA
LANE = 128
RQ = LANE // OA
NQ = OA // RQ
LIVE_AT = 64
CHUNKS = (4, 4)
BF = jnp.bfloat16
F4 = jnp.float32


def iota(shape, dim):
    return lax.broadcasted_iota(jnp.int32, shape, dim)


def mm(a, b):
    return lax.dot_general(a, b, (((1,), (0,)), ((), ())), preferred_element_type=F4)


def mm_nt(a, b):
    return lax.dot_general(a, b, (((1,), (1,)), ((), ())), preferred_element_type=F4)


def mm_tn(a, b):
    return lax.dot_general(a, b, (((0,), (0,)), ((), ())), preferred_element_type=F4)


def onehot(cond):
    return cond.astype(F4).astype(BF)


def div(x, n):
    if n & (n - 1) == 0:
        return lax.shift_right_logical(x, jnp.full_like(x, n.bit_length() - 1))
    return x // n


def mod(x, n):
    if n & (n - 1) == 0:
        return x & (n - 1)
    return x % n


def mm_split(a, b):
    count = a.shape[0]
    high = a.astype(BF)
    rest = a - high.astype(F4)
    middle = rest.astype(BF)
    low = (rest - middle.astype(F4)).astype(BF)
    out = mm(jnp.concatenate([high.astype(F4), middle.astype(F4), low.astype(F4)], axis=0).astype(BF), b)
    return out[:count] + out[count : 2 * count] + out[2 * count :]


def slot_onehot(pair_row):
    count = pair_row.shape[1]
    slot = iota((NAT * NAT, count), 0)
    second = mod(div(slot, NAT), 2) * RQ + div(slot, 2 * NAT)
    return mod(slot, NAT) * NAT + second == pair_row


def pair_row(pairs_ref, place_ref, step):
    at = mod(place_ref[1] + step, pairs_ref.shape[0])
    return pairs_ref[pl.ds(at, 1), :]


def to_matrix(tiles, swap):
    rows = [
        jnp.concatenate(
            [t[i * 2 * NAT : (i + 1) * 2 * NAT, q * LANE : (q + 1) * LANE] for i in range(RQ)],
            axis=1,
        )
        for t in tiles
        for q in range(NQ)
    ]
    mixed = mm(jnp.concatenate(rows, axis=0), swap)
    out = []
    for n in range(len(tiles)):
        part = mixed[n * 2 * NQ * NAT : (n + 1) * 2 * NQ * NAT]
        blocks = [
            jnp.concatenate(
                [
                    part[(q * 2 + g) * NAT : (q * 2 + g + 1) * NAT, i * LANE : (i + 1) * LANE]
                    for g in range(2)
                ],
                axis=1,
            )
            for i in range(RQ)
            for q in range(NQ)
        ]
        out.append(jnp.concatenate(blocks, axis=0).astype(BF))
    return out


def from_matrix(matrices, swap):
    rows = [
        jnp.concatenate(
            [
                m[(i * NQ + q) * NAT : (i * NQ + q + 1) * NAT, g * LANE : (g + 1) * LANE]
                for i in range(RQ)
            ],
            axis=1,
        )
        for m in matrices
        for q in range(NQ)
        for g in range(2)
    ]
    mixed = mm(jnp.concatenate(rows, axis=0).astype(BF), swap).astype(BF)
    out = []
    for n in range(len(matrices)):
        part = mixed[n * 2 * NQ * NAT : (n + 1) * 2 * NQ * NAT]
        out.append(
            jnp.concatenate(
                [
                    jnp.concatenate(
                        [
                            part[q * 2 * NAT : (q + 1) * 2 * NAT, i * LANE : (i + 1) * LANE]
                            for q in range(NQ)
                        ],
                        axis=1,
                    )
                    for i in range(RQ)
                ],
                axis=0,
            )
        )
    return out


def tables_kernel(
    occ_ref, vir_ref, screened_ref, live_ref, meta_ref, swap_ref, both_ref, cols_ref, vir_t_ref
):
    own_count = live_ref.shape[1]
    meta_ref[...] = jnp.zeros(meta_ref.shape, BF)
    meta_ref[:, : screened_ref.shape[1]] = screened_ref[...]
    meta_ref[:, LIVE_AT : LIVE_AT + own_count] = jnp.broadcast_to(
        live_ref[...].astype(F4), (BLK, own_count)
    ).astype(BF)
    size = RQ * LANE
    row = iota((size, size), 0)
    col = iota((size, size), 1)
    swapped = mod(div(row, OA), RQ) * LANE + div(row, LANE) * OA + mod(row, OA)
    swap_ref[...] = onehot(swapped == col)
    row = iota((NORB, NORB), 0)
    col = iota((NORB, NORB), 1)
    natural = mod(row, NAT) * OA + mod(div(row, NAT), NQ) * RQ + div(row, NAT * NQ)
    order = onehot(natural == col)
    occ = occ_ref[...]
    cols = mm_nt(occ, order).astype(BF)
    both = mm(order, cols)
    cols_ref[...] = cols
    both_ref[:NORB] = both.T.astype(BF)
    both_ref[NORB:] = both.astype(BF)
    vir_t_ref[...] = vir_ref[...].astype(F4).T.astype(BF)


def own_kernel(count, first, place_ref, pairs_ref, *refs):
    metas, pieces = refs[:count], refs[count : 2 * count]
    swap_ref, both_ref, cols_ref, vir_ref, vir_t_ref = refs[2 * count : 2 * count + 5]
    matrix_ref, right_ref, z_ref, y_ref = refs[2 * count + 5 :]
    group, own_count = matrix_ref.shape[0], pieces[0].shape[1]
    swap = swap_ref[...]
    selects = []
    for s in range(count):
        live = metas[s][0:1, LIVE_AT : LIVE_AT + own_count].astype(F4)
        select = slot_onehot(pair_row(pairs_ref, place_ref, s)).astype(F4)
        selects.append((select * live).astype(BF))
    tiles = []
    for p in range(group):
        total = mm(selects[0], pieces[0][first + p])
        for s in range(1, count):
            total = total + mm(selects[s], pieces[s][first + p])
        tiles.append(total.astype(BF))
    own_select = slot_onehot(pair_row(pairs_ref, place_ref, 0)).astype(F4).T.astype(BF)
    matrices = to_matrix(tiles, swap)
    right = mm(jnp.concatenate(matrices, axis=0), cols_ref[...]).astype(BF)
    both = both_ref[...]
    lefts = [mm(both, m).astype(BF) for m in matrices]
    z = mm(jnp.concatenate([left[:NORB] for left in lefts], axis=0), vir_ref[...])
    y = mm(jnp.concatenate([left[NORB:] for left in lefts], axis=0), vir_t_ref[...])
    for value, ref in ((z, z_ref), (y, y_ref)):
        parts = from_matrix([value[p * NORB : (p + 1) * NORB] for p in range(group)], swap)
        for p in range(group):
            ref[p * own_count : (p + 1) * own_count] = mm(own_select, parts[p]).astype(BF)
    for p in range(group):
        matrix_ref[p] = matrices[p]
        right_ref[p] = right[p * NORB : (p + 1) * NORB]


def window_kernel(lanes, sigma_scale, chi_scale, place_ref, *refs):
    (pairs_ref, meta0, meta1, meta2, tile0, tile1a, tile1b, tile2) = refs[:8]
    swap_ref, cols_ref = refs[8:10]
    own, (keep_ref, send_ref) = refs[10:-2], refs[-2:]
    matrices = [ref[p] for ref in own[::4] for p in range(ref.shape[0])]
    rights = [ref[p] for ref in own[1::4] for p in range(ref.shape[0])]
    z = jnp.concatenate([ref[...] for ref in own[2::4]], axis=0)
    y = jnp.concatenate([ref[...] for ref in own[3::4]], axis=0)
    pair_count, own_count = pairs_ref.shape
    rows = BLK * own_count
    block, pair_at = place_ref[0], place_ref[1]
    row = iota((rows, rows), 0)
    col = iota((rows, rows), 1)
    same = (mod(row, own_count) == mod(col, own_count)).astype(F4)
    spread_row, spread_col = iota((LANE, rows), 0), iota((LANE, rows), 1)
    spread = onehot(spread_row == LIVE_AT + mod(spread_col, own_count))
    metas = [m[...] for m in (meta0, meta1, meta2)]
    masks = [same * mm(m, spread)[0:1, :] for m in metas]
    tiles = [tile0[...], tile1a[...] + tile1b[...], tile2[...]]
    expand = onehot(div(iota((rows, BLK), 0), own_count) == iota((rows, BLK), 1))
    own_weights = mm(expand, metas[0]).astype(BF)
    mixed = jnp.zeros((rows, PAIR), F4)
    for t in range(REACH + 1):
        pick = onehot(spread_row == (REACH + t) * BLK + div(spread_col, own_count))
        mixed = mixed + mm((mm(own_weights, pick) * masks[t]).astype(BF), tiles[t])
    other = jnp.zeros((rows, PAIR), F4)
    unspread = onehot(iota((BLK, rows), 0) == div(iota((BLK, rows), 1), own_count))
    for t in range(1, REACH + 1):
        pick = onehot(
            iota((rows, LANE), 1) == (REACH - t) * BLK + div(iota((rows, LANE), 0), own_count)
        )
        weights = mm(mm_nt(pick, metas[t]).astype(BF), unspread)
        other = other + mm((weights * masks[t]).astype(BF), tiles[t])
    mixed = mixed.astype(BF)
    other = other.astype(BF)
    swap = swap_ref[...]
    own_select = onehot(slot_onehot(pair_row(pairs_ref, place_ref, 0)))
    parts = [
        mm(own_select, value[r * own_count : (r + 1) * own_count]).astype(BF)
        for value in (mixed, other)
        for r in range(BLK)
    ]
    values = to_matrix(parts, swap)
    scaled = mm(jnp.concatenate(values[:BLK], axis=0), cols_ref[...]).astype(BF)
    lefts = [scaled[r * NORB : (r + 1) * NORB] for r in range(BLK)]
    total = mm(
        jnp.concatenate(lefts + rights, axis=1),
        jnp.concatenate(matrices + values[BLK:], axis=0),
    )
    total = total * -sigma_scale
    high = total.astype(BF).astype(F4)
    parts = from_matrix([high, total - high], swap)
    parity = block & 1
    half = own_count // 2
    for s in range(pair_count):
        select = onehot(slot_onehot(pair_row(pairs_ref, place_ref, s)))
        owned = mm_tn(select, parts[0]) + mm_tn(select, parts[1])
        first, second = owned[:half], owned[half:]
        keep = jnp.where(parity == 0, first, second)
        send = jnp.where(parity == 0, second, first)
        for q in range(NQ):
            keep_ref[s, q * half : (q + 1) * half, :] = keep[:, q * LANE : (q + 1) * LANE]
            send_ref[s, q * half : (q + 1) * half, :] = send[:, q * LANE : (q + 1) * LANE]

    chi = jnp.zeros((BLK, LANE), F4)
    for t in range(-REACH, REACH + 1):
        w = abs(t)
        if t < 0:
            cross = mm_nt(tiles[w], y)
        else:
            cross = mm_nt(z, tiles[w])
        cross = cross * masks[w]
        sums = jnp.concatenate(
            [
                jnp.sum(cross[p * own_count : (p + 1) * own_count], axis=0, keepdims=True)
                for p in range(BLK)
            ],
            axis=0,
        )
        pick = onehot(
            iota((rows, LANE), 1) == (REACH + t) * BLK + div(iota((rows, LANE), 0), own_count)
        )
        chi = chi + mm_split(sums, pick)
    chi = chi * chi_scale
    share = (2 * REACH + 1) * BLK // pair_count
    column = iota((LANE, 1), 0)
    target = block + jnp.maximum(REACH - div(column, BLK), 0)
    at_pair = jnp.zeros((LANE, 1), jnp.int32)
    for s in range(1, pair_count):
        at_pair = at_pair + (column >= s * share).astype(jnp.int32)
    place = mod(at_pair - pair_at + pair_count, pair_count) + (
        ((target ^ block) & 1) * pair_count
    )
    spot = place * lanes + div(target, 2) * share + column - at_pair * share
    spread = onehot(iota((LANE, 2 * pair_count * lanes), 1) == spot)
    placed = mm_split(chi, spread)
    for s in range(pair_count):
        for i in range(lanes // LANE):
            at = slice(NQ * half + i * BLK, NQ * half + (i + 1) * BLK)
            begin = s * lanes + i * LANE
            keep_ref[s, at, :] = placed[:, begin : begin + LANE]
            begin += pair_count * lanes
            send_ref[s, at, :] = placed[:, begin : begin + LANE]


def last_kernel(place_ref, own_ref, other_ref, chi_ref, energy_ref):
    half = energy_ref.shape[0] // 2
    share = chi_ref.shape[1]
    parity = place_ref[0] & 1
    own, other = own_ref[...], other_ref[...]
    first = jnp.where(parity == 0, own, other)
    second = jnp.where(parity == 0, other, own)
    for q in range(NQ):
        at = slice(q * LANE, (q + 1) * LANE)
        energy_ref[:half, at] = first[q * half : (q + 1) * half]
        energy_ref[half:, at] = second[q * half : (q + 1) * half]
    start = (place_ref[0] >> 1) * share
    total = None
    for i in range((own.shape[0] - NQ * half) // BLK):
        chi = own[NQ * half + i * BLK : NQ * half + (i + 1) * BLK]
        pick = onehot(iota((LANE, LANE), 0) + i * LANE == start + iota((LANE, LANE), 1))
        part = mm_split(chi, pick)
        total = part if total is None else total + part
    chi_ref[...] = total[:, :share]


def call(body, outs, *args, flops=10**8):
    full = pl.BlockSpec(memory_space=pltpu.VMEM)
    return pl.pallas_call(
        body,
        out_shape=outs,
        in_specs=[pl.BlockSpec(memory_space=pltpu.SMEM) if a.ndim == 1 else full for a in args],
        out_specs=jax.tree.map(lambda o: full, outs),
        cost_estimate=pl.CostEstimate(flops=flops, bytes_accessed=10**6, transcendentals=0),
        compiler_params=pltpu.CompilerParams(vmem_limit_bytes=24 << 20),
    )(*args)


def per_device(three_center, tile_live, pair_atoms, green_occ, green_vir, screened):
    block_rows, own_count = three_center.shape[:2]
    aux_count, pair_count = lax.axis_size("aux"), lax.axis_size("pair")
    block, pair_at = lax.axis_index("aux"), lax.axis_index("pair")
    rows = block_rows * own_count
    window = screened.shape[1]
    shape = jax.ShapeDtypeStruct

    def shifted(value, steps, parity=None):
        return lax.ppermute(
            value,
            "aux",
            [
                (s, s + steps)
                for s in range(aux_count)
                if 0 <= s + steps < aux_count and parity in (None, s % 2)
            ],
        )

    def turned(value, steps):
        return lax.ppermute(
            value, "pair", [(s, (s - steps) % pair_count) for s in range(pair_count)]
        )

    def flipped(value, mask):
        return lax.ppermute(value, "aux", [(s, s ^ mask) for s in range(aux_count)])

    far = shifted(three_center, -2)
    firsts = [sum(CHUNKS[:c]) for c in range(len(CHUNKS))]
    pieces = [three_center] + [turned(three_center, s) for s in range(1, pair_count)]
    near_even = shifted(three_center, -1, 1)
    square = shape((NORB, NORB), BF)
    meta, swap, both, cols, vir_t = call(
        tables_kernel,
        [
            shape((block_rows, LANE), BF),
            shape((RQ * LANE, RQ * LANE), BF),
            shape((2 * NORB, NORB), BF),
            square,
            square,
        ],
        green_occ,
        green_vir,
        screened,
        tile_live,
    )
    metas = [meta] + [turned(meta, s) for s in range(1, pair_count)]
    meta_near = shifted(meta, -1)
    meta_far = shifted(meta, -2)
    near_odd = shifted(far, 1, 0)
    pairs = pair_atoms.reshape(pair_count, own_count)
    place = jnp.stack([block, pair_at]).astype(jnp.int32)
    own = []
    for c, first in enumerate(firsts):
        own.append(
            call(
                lambda *refs, first=first: own_kernel(pair_count, first, *refs),
                [
                    shape((CHUNKS[c], NORB, NORB), BF),
                    shape((CHUNKS[c], NORB, NORB), BF),
                    shape((CHUNKS[c] * own_count, PAIR), BF),
                    shape((CHUNKS[c] * own_count, PAIR), BF),
                ],
                place,
                pairs,
                *metas,
                *pieces,
                swap,
                both,
                cols,
                green_vir,
                vir_t,
            )
        )

    lanes = -(-(aux_count // 2) * (window // pair_count) // LANE) * LANE
    message = shape((pair_count, own_count // 2 * NQ + lanes // LANE * BLK, LANE), F4)
    aux_total = block_rows * aux_count
    keep, send = call(
        lambda *refs: window_kernel(
            lanes, 1.0 / math.sqrt(aux_total * NAT * OA * NAT), 1.0 / (OA * NAT), *refs
        ),
        [message, message],
        place,
        pairs,
        meta,
        meta_near,
        meta_far,
        three_center.reshape(rows, PAIR),
        near_even.reshape(rows, PAIR),
        near_odd.reshape(rows, PAIR),
        far.reshape(rows, PAIR),
        swap,
        cols,
        *[value for values in own for value in values],
    )
    total = keep + flipped(send, 1)
    owned = total[0]
    for s in range(1, pair_count):
        owned = owned + turned(total[s], -s)
    mask = 2
    while mask < aux_count:
        owned = owned + flipped(owned, mask)
        mask *= 2
    polarizability, self_energy = call(
        last_kernel,
        [
            shape((block_rows, window // pair_count), F4),
            shape((own_count, PAIR), F4),
        ],
        place,
        owned,
        flipped(owned, 1),
    )
    return polarizability, self_energy


def solution(mesh):
    placed = (P("aux", "pair", None), P("aux", "pair"), P(), P(), P(), P("aux", None))
    return jax.shard_map(
        per_device,
        mesh=mesh,
        in_specs=placed,
        out_specs=(P("aux", "pair"), P("pair", None)),
        check_vma=False,
    )
```

```python
import math

import jax
import jax.numpy as jnp
from jax import lax
from jax.experimental import pallas as pl
from jax.experimental.pallas import tpu as pltpu
from jax.sharding import PartitionSpec as P


OA = 32
NAT = 8
REACH = 2
BLK = 8
NORB = OA * NAT
PAIR = OA * OA
LANE = 128
RQ = LANE // OA
NQ = OA // RQ
LIVE_AT = 64
CHUNKS = (4, 4)
BF = jnp.bfloat16
F4 = jnp.float32


def iota(shape, dim):
    return lax.broadcasted_iota(jnp.int32, shape, dim)


def mm(a, b):
    return lax.dot_general(a, b, (((1,), (0,)), ((), ())), preferred_element_type=F4)


def mm_nt(a, b):
    return lax.dot_general(a, b, (((1,), (1,)), ((), ())), preferred_element_type=F4)


def mm_tn(a, b):
    return lax.dot_general(a, b, (((0,), (0,)), ((), ())), preferred_element_type=F4)


def onehot(cond):
    return cond.astype(F4).astype(BF)


def div(x, n):
    if n & (n - 1) == 0:
        return lax.shift_right_logical(x, jnp.full_like(x, n.bit_length() - 1))
    return x // n


def mod(x, n):
    if n & (n - 1) == 0:
        return x & (n - 1)
    return x % n


def mm_split(a, b):
    count = a.shape[0]
    high = a.astype(BF)
    rest = a - high.astype(F4)
    middle = rest.astype(BF)
    low = (rest - middle.astype(F4)).astype(BF)
    out = mm(jnp.concatenate([high.astype(F4), middle.astype(F4), low.astype(F4)], axis=0).astype(BF), b)
    return out[:count] + out[count : 2 * count] + out[2 * count :]


def slot_onehot(pair_row):
    count = pair_row.shape[1]
    slot = iota((NAT * NAT, count), 0)
    second = mod(div(slot, NAT), 2) * RQ + div(slot, 2 * NAT)
    return mod(slot, NAT) * NAT + second == pair_row


def pair_row(pairs_ref, place_ref, step, own_count):
    count = pairs_ref.shape[1] // own_count
    at = mod(place_ref[1] + step, count)
    row = jnp.zeros((1, own_count), jnp.int32)
    for s in range(count):
        row = jnp.where(at == s, pairs_ref[0:1, s * own_count : (s + 1) * own_count], row)
    return row


def swap_blocks(parts):
    lane = iota(parts[0].shape, 1)
    low = lane < LANE // 2
    even = mod(lane, LANE // 2) < OA
    a, b, c, d = parts
    a, c = jnp.where(low, a, pltpu.roll(c, LANE // 2, 1)), jnp.where(low, pltpu.roll(a, LANE // 2, 1), c)
    b, d = jnp.where(low, b, pltpu.roll(d, LANE // 2, 1)), jnp.where(low, pltpu.roll(b, LANE // 2, 1), d)
    a, b = jnp.where(even, a, pltpu.roll(b, OA, 1)), jnp.where(even, pltpu.roll(a, LANE - OA, 1), b)
    c, d = jnp.where(even, c, pltpu.roll(d, OA, 1)), jnp.where(even, pltpu.roll(c, LANE - OA, 1), d)
    return a, b, c, d


def to_matrix(tiles):
    parts = [
        jnp.concatenate(
            [tiles[i * 2 * NAT : (i + 1) * 2 * NAT, q * LANE : (q + 1) * LANE] for q in range(NQ)],
            axis=0,
        )
        for i in range(RQ)
    ]
    parts = [part.astype(F4) for part in swap_blocks(parts)]
    out = [
        jnp.concatenate(
            [part[(q * 2 + g) * NAT : (q * 2 + g + 1) * NAT] for g in range(2)], axis=1
        )
        for part in parts
        for q in range(NQ)
    ]
    return jnp.concatenate(out, axis=0).astype(BF)


def from_matrix(matrix):
    parts = [
        jnp.concatenate(
            [
                matrix[(i * NQ + q) * NAT : (i * NQ + q + 1) * NAT, g * LANE : (g + 1) * LANE]
                for q in range(NQ)
                for g in range(2)
            ],
            axis=0,
        ).astype(BF)
        for i in range(RQ)
    ]
    return jnp.concatenate(
        [
            jnp.concatenate(
                [part[q * 2 * NAT : (q + 1) * 2 * NAT] for q in range(NQ)], axis=1
            )
            for part in swap_blocks(parts)
        ],
        axis=0,
    )


def tables_kernel(*refs):
    ins, outs = refs[:6], refs[6:-5]
    pairs_ref, vir_ref, meta_ref, both_ref, cols_ref, vir_t_ref = outs[:6]
    parts = outs[6:]
    occ_ref, screened_ref, live_ref, whole_ref, sems = refs[-5:]
    targets = (occ_ref, vir_ref, screened_ref, live_ref, pairs_ref, whole_ref)
    copies = [
        pltpu.make_async_copy(a, b, sems.at[i]) for i, (a, b) in enumerate(zip(ins, targets))
    ]
    for copy in copies:
        copy.start()
    for copy in copies[:-1]:
        copy.wait()
    own_count = live_ref.shape[1]
    meta_ref[...] = jnp.zeros(meta_ref.shape, BF)
    meta_ref[:, : screened_ref.shape[1]] = screened_ref[...]
    meta_ref[:, LIVE_AT : LIVE_AT + own_count] = jnp.broadcast_to(
        live_ref[...].astype(F4), (BLK, own_count)
    ).astype(BF)
    row = iota((NORB, NORB), 0)
    col = iota((NORB, NORB), 1)
    natural = mod(row, NAT) * OA + mod(div(row, NAT), NQ) * RQ + div(row, NAT * NQ)
    order = onehot(natural == col)
    occ = occ_ref[...]
    cols = mm_nt(occ, order).astype(BF)
    both = mm(order, cols)
    cols_ref[...] = cols
    both_ref[:NORB] = both.T.astype(BF)
    both_ref[NORB:] = both.astype(BF)
    vir_t_ref[...] = vir_ref[...].astype(F4).T.astype(BF)
    diagonal = iota((own_count, own_count), 0) == iota((own_count, own_count), 1)
    live = jnp.where(diagonal, live_ref[...].astype(F4), 0.0)
    live = jnp.sum(live, axis=1, keepdims=True).astype(BF)
    copies[-1].wait()
    at = 0
    for ref in parts:
        for p in range(ref.shape[0] // own_count):
            ref[p * own_count : (p + 1) * own_count] = whole_ref[at] * live
            at += 1


def own_kernel(count, own_count, place_ref, pairs_ref, *refs):
    pieces = refs[:count]
    both_ref, cols_ref, vir_ref, vir_t_ref = refs[count : count + 4]
    matrix_ref, right_ref, z_ref, y_ref = refs[count + 4 :]
    group = matrix_ref.shape[0]
    selects = [
        onehot(slot_onehot(pair_row(pairs_ref, place_ref, s, own_count))) for s in range(count)
    ]
    tiles = []
    for p in range(group):
        at = slice(p * own_count, (p + 1) * own_count)
        total = mm(selects[0], pieces[0][at])
        for s in range(1, count):
            total = total + mm(selects[s], pieces[s][at])
        tiles.append(total.astype(BF))
    own_select = slot_onehot(pair_row(pairs_ref, place_ref, 0, own_count)).astype(F4).T.astype(BF)
    matrices = [to_matrix(t) for t in tiles]
    right = mm(jnp.concatenate(matrices, axis=0), cols_ref[...]).astype(BF)
    both = both_ref[...]
    lefts = [mm(both, m).astype(BF) for m in matrices]
    z = mm(jnp.concatenate([left[:NORB] for left in lefts], axis=0), vir_ref[...])
    y = mm(jnp.concatenate([left[NORB:] for left in lefts], axis=0), vir_t_ref[...])
    for value, ref in ((z, z_ref), (y, y_ref)):
        for p in range(group):
            part = from_matrix(value[p * NORB : (p + 1) * NORB])
            ref[p * own_count : (p + 1) * own_count] = mm(own_select, part).astype(BF)
    for p in range(group):
        matrix_ref[p] = matrices[p]
        right_ref[p] = right[p * NORB : (p + 1) * NORB]


def window_kernel(lanes, sigma_scale, chi_scale, place_ref, *refs):
    (pairs_ref, meta0, meta1, meta2, tile1a, tile1b, tile2, cols_ref) = refs[:8]
    keep_ref, send_ref, near_ref, mixed_ref, other_ref = refs[-5:]
    own, tile0 = refs[8 : 8 + 4 * len(CHUNKS)], refs[8 + 4 * len(CHUNKS) : -5]
    matrices = [ref[p] for ref in own[::4] for p in range(ref.shape[0])]
    rights = [ref[p] for ref in own[1::4] for p in range(ref.shape[0])]
    z = jnp.concatenate([ref[...] for ref in own[2::4]], axis=0)
    y = jnp.concatenate([ref[...] for ref in own[3::4]], axis=0)
    own_count = tile2.shape[0] // BLK
    pair_count = pairs_ref.shape[1] // own_count
    rows = BLK * own_count
    block, pair_at = place_ref[0], place_ref[1]
    row = iota((rows, rows), 0)
    col = iota((rows, rows), 1)
    same = (mod(row, own_count) == mod(col, own_count)).astype(F4)
    spread_row, spread_col = iota((LANE, rows), 0), iota((LANE, rows), 1)
    spread = onehot(spread_row == LIVE_AT + mod(spread_col, own_count))
    metas = [m[...] for m in (meta0, meta1, meta2)]
    masks = [same * mm(m, spread)[0:1, :] for m in metas]
    near_ref[...] = tile1a[...] + tile1b[...]
    tiles = [jnp.concatenate([t[...] for t in tile0], axis=0), near_ref, tile2]

    def spread_rows(value):
        return jnp.concatenate(
            [jnp.broadcast_to(value[p : p + 1], (own_count, rows)) for p in range(BLK)], axis=0
        )

    mixed = jnp.zeros((rows, PAIR), F4)
    for t in range(REACH + 1):
        pick = onehot(spread_row == (REACH + t) * BLK + div(spread_col, own_count))
        weight = spread_rows(mm(metas[0], pick)) * masks[t]
        mixed = mixed + mm(weight.astype(BF), tiles[t][...])
    mixed_ref[...] = mixed.astype(BF)
    other = jnp.zeros((rows, PAIR), F4)
    unspread = onehot(iota((BLK, rows), 0) == div(iota((BLK, rows), 1), own_count))
    for t in range(1, REACH + 1):
        pick = onehot(iota((BLK, LANE), 1) == (REACH - t) * BLK + iota((BLK, LANE), 0))
        weight = spread_rows(mm(mm_nt(pick, metas[t]).astype(BF), unspread)) * masks[t]
        other = other + mm(weight.astype(BF), tiles[t][...])
    other_ref[...] = other.astype(BF)
    own_select = onehot(slot_onehot(pair_row(pairs_ref, place_ref, 0, own_count)))

    def chi_part(steps):
        crosses = []
        for t in steps:
            w = abs(t)
            if t < 0:
                crosses.append(mm_nt(tiles[w][...], y))
            else:
                crosses.append(mm_nt(z, tiles[w][...]))
        sums, picks = [], []
        for t, cross in zip(steps, crosses):
            cross = cross * masks[abs(t)]
            sums.append(
                jnp.concatenate(
                    [
                        jnp.sum(cross[p * own_count : (p + 1) * own_count], axis=0, keepdims=True)
                        for p in range(BLK)
                    ],
                    axis=0,
                )
            )
            picks.append(
                onehot(
                    iota((rows, LANE), 1)
                    == (REACH + t) * BLK + div(iota((rows, LANE), 0), own_count)
                )
            )
        return mm_split(jnp.concatenate(sums, axis=1), jnp.concatenate(picks, axis=0))

    parts = [
        mm(own_select, ref[r * own_count : (r + 1) * own_count]).astype(BF)
        for ref in (mixed_ref, other_ref)
        for r in range(BLK)
    ]
    values = [to_matrix(part) for part in parts]
    chi = chi_part((-2, 2)) + chi_part((-1, 1)) + chi_part((0,))
    scaled = mm(jnp.concatenate(values[:BLK], axis=0), cols_ref[...]).astype(BF)
    lefts = [scaled[r * NORB : (r + 1) * NORB] for r in range(BLK)]
    total = mm(jnp.concatenate(lefts, axis=1), jnp.concatenate(matrices, axis=0))
    total = total + mm(jnp.concatenate(rights, axis=1), jnp.concatenate(values[BLK:], axis=0))
    total = total * -sigma_scale
    high = total.astype(BF).astype(F4)
    parts = [from_matrix(high), from_matrix(total - high)]
    parity = block & 1
    half = own_count // 2
    for s in range(pair_count):
        select = onehot(slot_onehot(pair_row(pairs_ref, place_ref, s, own_count)))
        owned = mm_tn(select, parts[0]) + mm_tn(select, parts[1])
        first, second = owned[:half], owned[half:]
        keep = jnp.where(parity == 0, first, second)
        send = jnp.where(parity == 0, second, first)
        for q in range(NQ):
            keep_ref[s, q * half : (q + 1) * half, :] = keep[:, q * LANE : (q + 1) * LANE]
            send_ref[s, q * half : (q + 1) * half, :] = send[:, q * LANE : (q + 1) * LANE]

    chi = chi * chi_scale
    share = (2 * REACH + 1) * BLK // pair_count
    column = iota((LANE, 1), 0)
    target = block + jnp.maximum(REACH - div(column, BLK), 0)
    at_pair = jnp.zeros((LANE, 1), jnp.int32)
    for s in range(1, pair_count):
        at_pair = at_pair + (column >= s * share).astype(jnp.int32)
    place = mod(at_pair - pair_at + pair_count, pair_count) + (
        ((target ^ block) & 1) * pair_count
    )
    spot = place * lanes + div(target, 2) * share + column - at_pair * share
    spread = onehot(iota((LANE, 2 * pair_count * lanes), 1) == spot)
    placed = mm_split(chi, spread)
    for s in range(pair_count):
        for i in range(lanes // LANE):
            at = slice(NQ * half + i * BLK, NQ * half + (i + 1) * BLK)
            begin = s * lanes + i * LANE
            keep_ref[s, at, :] = placed[:, begin : begin + LANE]
            begin += pair_count * lanes
            send_ref[s, at, :] = placed[:, begin : begin + LANE]


def last_kernel(place_ref, own_ref, other_ref, chi_ref, energy_ref):
    half = energy_ref.shape[0] // 2
    share = chi_ref.shape[1]
    parity = place_ref[0] & 1
    own, other = own_ref[...], other_ref[...]
    first = jnp.where(parity == 0, own, other)
    second = jnp.where(parity == 0, other, own)
    for q in range(NQ):
        at = slice(q * LANE, (q + 1) * LANE)
        energy_ref[:half, at] = first[q * half : (q + 1) * half]
        energy_ref[half:, at] = second[q * half : (q + 1) * half]
    start = (place_ref[0] >> 1) * share
    total = None
    for i in range((own.shape[0] - NQ * half) // BLK):
        chi = own[NQ * half + i * BLK : NQ * half + (i + 1) * BLK]
        pick = onehot(iota((LANE, LANE), 0) + i * LANE == start + iota((LANE, LANE), 1))
        part = mm_split(chi, pick)
        total = part if total is None else total + part
    chi_ref[...] = total[:, :share]


def call(body, outs, *args, scratch=(), ins=None, flops=10**8):
    full = pl.BlockSpec(memory_space=pltpu.VMEM)
    ins = ins or full
    if ins is not full:
        args = [pltpu.with_memory_space_constraint(a, pltpu.HBM) for a in args]
    return pl.pallas_call(
        body,
        out_shape=outs,
        in_specs=[pl.BlockSpec(memory_space=pltpu.SMEM) if a.ndim == 1 else ins for a in args],
        out_specs=jax.tree.map(lambda o: full, outs),
        scratch_shapes=scratch,
        cost_estimate=pl.CostEstimate(flops=flops, bytes_accessed=10**6, transcendentals=0),
        compiler_params=pltpu.CompilerParams(vmem_limit_bytes=24 << 20),
    )(*args)


def per_device(three_center, tile_live, pair_atoms, green_occ, green_vir, screened):
    block_rows, own_count = three_center.shape[:2]
    aux_count, pair_count = lax.axis_size("aux"), lax.axis_size("pair")
    block, pair_at = lax.axis_index("aux"), lax.axis_index("pair")
    rows = block_rows * own_count
    window = screened.shape[1]
    shape = jax.ShapeDtypeStruct

    def shifted(value, steps, parity=None):
        return lax.ppermute(
            value,
            "aux",
            [
                (s, s + steps)
                for s in range(aux_count)
                if 0 <= s + steps < aux_count and parity in (None, s % 2)
            ],
        )

    def turned(value, steps):
        return lax.ppermute(
            value, "pair", [(s, (s - steps) % pair_count) for s in range(pair_count)]
        )

    def flipped(value, mask):
        return lax.ppermute(value, "aux", [(s, s ^ mask) for s in range(aux_count)])

    far = shifted(three_center, -2)
    near_even = shifted(three_center, -1, 1)
    square = shape((NORB, NORB), BF)
    pairs, vir, meta, both, cols, vir_t, *parts = call(
        tables_kernel,
        [
            shape((1, pair_count * own_count), jnp.int32),
            square,
            shape((block_rows, LANE), BF),
            shape((2 * NORB, NORB), BF),
            square,
            square,
        ]
        + [shape((c * own_count, PAIR), BF) for c in CHUNKS],
        green_occ,
        green_vir,
        screened,
        tile_live,
        pair_atoms.reshape(1, pair_count * own_count),
        three_center,
        scratch=[
            pltpu.VMEM((NORB, NORB), BF),
            pltpu.VMEM(screened.shape, BF),
            pltpu.VMEM(tile_live.shape, jnp.int32),
            pltpu.VMEM(three_center.shape, BF),
            pltpu.SemaphoreType.DMA((6,)),
        ],
        ins=pl.BlockSpec(memory_space=pltpu.HBM),
    )
    pieces = []
    for part in parts:
        pieces.append([part] + [turned(part, s) for s in range(1, pair_count)])
    meta_near = shifted(meta, -1)
    meta_far = shifted(meta, -2)
    near_odd = shifted(far, 1, 0)
    place = jnp.stack([block, pair_at]).astype(jnp.int32)
    own = []
    for c, count in enumerate(CHUNKS):
        own += call(
            lambda *refs: own_kernel(pair_count, own_count, *refs),
            [
                shape((count, NORB, NORB), BF),
                shape((count, NORB, NORB), BF),
                shape((count * own_count, PAIR), BF),
                shape((count * own_count, PAIR), BF),
            ],
            place,
            pairs,
            *pieces[c],
            both,
            cols,
            vir,
            vir_t,
        )

    lanes = -(-(aux_count // 2) * (window // pair_count) // LANE) * LANE
    message = shape((pair_count, own_count // 2 * NQ + lanes // LANE * BLK, LANE), F4)
    aux_total = block_rows * aux_count
    keep, send = call(
        lambda *refs: window_kernel(
            lanes, 1.0 / math.sqrt(aux_total * NAT * OA * NAT), 1.0 / (OA * NAT), *refs
        ),
        [message, message],
        place,
        pairs,
        meta,
        meta_near,
        meta_far,
        near_even.reshape(rows, PAIR),
        near_odd.reshape(rows, PAIR),
        far.reshape(rows, PAIR),
        cols,
        *own,
        *parts,
        scratch=[pltpu.VMEM((rows, PAIR), BF)] * 3,
    )
    total = keep + flipped(send, 1)
    owned = total[0]
    for s in range(1, pair_count):
        owned = owned + turned(total[s], -s)
    masks = [1 << i for i in range(1, (aux_count - 1).bit_length())]
    for even, odd in zip(masks, masks[1:] + masks[:1]):
        owned = owned + lax.ppermute(
            owned, "aux", [(s, s ^ (odd if s % 2 else even)) for s in range(aux_count)]
        )
    polarizability, self_energy = call(
        last_kernel,
        [
            shape((block_rows, window // pair_count), F4),
            shape((own_count, PAIR), F4),
        ],
        place,
        owned,
        flipped(owned, 1),
    )
    return polarizability, self_energy


def solution(mesh):
    placed = (P("aux", "pair", None), P("aux", "pair"), P(), P(), P(), P("aux", None))
    return jax.shard_map(
        per_device,
        mesh=mesh,
        in_specs=placed,
        out_specs=(P("aux", "pair"), P("pair", None)),
        check_vma=False,
    )
```

```python
import math

import jax
import jax.numpy as jnp
from jax import lax
from jax.experimental import pallas as pl
from jax.experimental.pallas import tpu as pltpu
from jax.sharding import PartitionSpec as P


OA = 32
NAT = 8
REACH = 2
BLK = 8
NORB = OA * NAT
PAIR = OA * OA
LANE = 128
RQ = LANE // OA
NQ = OA // RQ
LIVE_AT = 64
CHUNKS = (4, 4)
BF = jnp.bfloat16
F4 = jnp.float32


def iota(shape, dim):
    return lax.broadcasted_iota(jnp.int32, shape, dim)


def mm(a, b):
    return lax.dot_general(a, b, (((1,), (0,)), ((), ())), preferred_element_type=F4)


def mm_nt(a, b):
    return lax.dot_general(a, b, (((1,), (1,)), ((), ())), preferred_element_type=F4)


def onehot(cond):
    return cond.astype(F4).astype(BF)


def div(x, n):
    if n & (n - 1) == 0:
        return lax.shift_right_logical(x, jnp.full_like(x, n.bit_length() - 1))
    return x // n


def mod(x, n):
    if n & (n - 1) == 0:
        return x & (n - 1)
    return x % n


def mm_split(a, b):
    count = a.shape[0]
    high = a.astype(BF)
    rest = a - high.astype(F4)
    middle = rest.astype(BF)
    low = (rest - middle.astype(F4)).astype(BF)
    out = mm(jnp.concatenate([high.astype(F4), middle.astype(F4), low.astype(F4)], axis=0).astype(BF), b)
    return out[:count] + out[count : 2 * count] + out[2 * count :]


def slot_onehot(pair_row):
    count = pair_row.shape[1]
    slot = iota((NAT * NAT, count), 0)
    second = mod(div(slot, NAT), 2) * RQ + div(slot, 2 * NAT)
    return mod(slot, NAT) * NAT + second == pair_row


def pair_row(pairs_ref, place_ref, step, own_count):
    count = pairs_ref.shape[1] // own_count
    at = mod(place_ref[1] + step, count)
    row = jnp.zeros((1, own_count), jnp.int32)
    for s in range(count):
        row = jnp.where(at == s, pairs_ref[0:1, s * own_count : (s + 1) * own_count], row)
    return row


def swap_blocks(parts):
    lane = iota(parts[0].shape, 1)
    low = lane < LANE // 2
    even = mod(lane, LANE // 2) < OA
    a, b, c, d = parts
    moved = pltpu.roll(jnp.where(low, c, a), LANE // 2, 1)
    a, c = jnp.where(low, a, moved), jnp.where(low, moved, c)
    moved = pltpu.roll(jnp.where(low, d, b), LANE // 2, 1)
    b, d = jnp.where(low, b, moved), jnp.where(low, moved, d)
    a, b = jnp.where(even, a, pltpu.roll(b, OA, 1)), jnp.where(even, pltpu.roll(a, LANE - OA, 1), b)
    c, d = jnp.where(even, c, pltpu.roll(d, OA, 1)), jnp.where(even, pltpu.roll(c, LANE - OA, 1), d)
    return a, b, c, d


def to_matrix(tiles):
    parts = [
        jnp.concatenate(
            [tiles[i * 2 * NAT : (i + 1) * 2 * NAT, q * LANE : (q + 1) * LANE] for q in range(NQ)],
            axis=0,
        )
        for i in range(RQ)
    ]
    parts = [part.astype(F4) for part in swap_blocks(parts)]
    out = [
        jnp.concatenate(
            [part[(q * 2 + g) * NAT : (q * 2 + g + 1) * NAT] for g in range(2)], axis=1
        )
        for part in parts
        for q in range(NQ)
    ]
    return jnp.concatenate(out, axis=0).astype(BF)


def from_matrix(matrix):
    parts = [
        jnp.concatenate(
            [
                matrix[(i * NQ + q) * NAT : (i * NQ + q + 1) * NAT, g * LANE : (g + 1) * LANE]
                for q in range(NQ)
                for g in range(2)
            ],
            axis=0,
        ).astype(BF)
        for i in range(RQ)
    ]
    return jnp.concatenate(
        [
            jnp.concatenate(
                [part[q * 2 * NAT : (q + 1) * 2 * NAT] for q in range(NQ)], axis=1
            )
            for part in swap_blocks(parts)
        ],
        axis=0,
    )


def tables_kernel(*refs):
    ins, outs = refs[:6], refs[6:-5]
    pairs_ref, vir_ref, meta_ref, both_ref, cols_ref, vir_t_ref = outs[:6]
    parts = outs[6:]
    occ_ref, screened_ref, live_ref, whole_ref, sems = refs[-5:]
    targets = (occ_ref, vir_ref, screened_ref, live_ref, pairs_ref, whole_ref)
    copies = [
        pltpu.make_async_copy(a, b, sems.at[i]) for i, (a, b) in enumerate(zip(ins, targets))
    ]
    for copy in copies:
        copy.start()
    for copy in copies[:-1]:
        copy.wait()
    own_count = live_ref.shape[1]
    meta_ref[...] = jnp.zeros(meta_ref.shape, BF)
    meta_ref[:, : screened_ref.shape[1]] = screened_ref[...]
    meta_ref[:, LIVE_AT : LIVE_AT + own_count] = jnp.broadcast_to(
        live_ref[...].astype(F4), (BLK, own_count)
    ).astype(BF)
    row = iota((NORB, NORB), 0)
    col = iota((NORB, NORB), 1)
    natural = mod(row, NAT) * OA + mod(div(row, NAT), NQ) * RQ + div(row, NAT * NQ)
    order = onehot(natural == col)
    occ = occ_ref[...]
    cols = mm_nt(occ, order).astype(BF)
    both = mm(order, cols)
    cols_ref[...] = cols
    both_ref[:NORB] = both.T.astype(BF)
    both_ref[NORB:] = both.astype(BF)
    vir_t_ref[...] = vir_ref[...].astype(F4).T.astype(BF)
    diagonal = iota((own_count, own_count), 0) == iota((own_count, own_count), 1)
    live = jnp.where(diagonal, live_ref[...].astype(F4), 0.0)
    live = jnp.sum(live, axis=1, keepdims=True).astype(BF)
    copies[-1].wait()
    at = 0
    for ref in parts:
        for p in range(ref.shape[0] // own_count):
            ref[p * own_count : (p + 1) * own_count] = whole_ref[at] * live
            at += 1


def own_kernel(count, own_count, place_ref, pairs_ref, *refs):
    pieces = refs[:count]
    both_ref, cols_ref, vir_ref, vir_t_ref = refs[count : count + 4]
    matrix_ref, right_ref, z_ref, y_ref = refs[count + 4 :]
    group = matrix_ref.shape[0]
    selects = [
        onehot(slot_onehot(pair_row(pairs_ref, place_ref, s, own_count))) for s in range(count)
    ]
    tiles = []
    for p in range(group):
        at = slice(p * own_count, (p + 1) * own_count)
        total = mm(selects[0], pieces[0][at])
        for s in range(1, count):
            total = total + mm(selects[s], pieces[s][at])
        tiles.append(total.astype(BF))
    own_select = slot_onehot(pair_row(pairs_ref, place_ref, 0, own_count)).astype(F4).T.astype(BF)
    matrices = [to_matrix(t) for t in tiles]
    both = both_ref[...]

    def transformed(rows, side):
        lefts = [mm(both[rows], m).astype(BF) for m in matrices]
        value = mm(jnp.concatenate(lefts, axis=0), side)
        return [value[p * NORB : (p + 1) * NORB] for p in range(group)]

    def selected(value, ref):
        for p in range(group):
            part = from_matrix(value[p])
            ref[p * own_count : (p + 1) * own_count] = mm(own_select, part).astype(BF)

    z = transformed(slice(0, NORB), vir_ref[...])
    y = transformed(slice(NORB, 2 * NORB), vir_t_ref[...])
    selected(z, z_ref)
    right = mm(jnp.concatenate(matrices, axis=0), cols_ref[...]).astype(BF)
    for p in range(group):
        matrix_ref[p] = matrices[p]
        right_ref[p] = right[p * NORB : (p + 1) * NORB]
    selected(y, y_ref)


def window_kernel(lanes, sigma_scale, chi_scale, place_ref, *refs):
    (pairs_ref, meta0, meta1, meta2, tile1a, tile1b, tile2, cols_ref) = refs[:8]
    keep_ref, send_ref, near_ref, mixed_ref, other_ref = refs[-5:]
    own, tile0 = refs[8 : 8 + 4 * len(CHUNKS)], refs[8 + 4 * len(CHUNKS) : -5]
    matrices = [ref[p] for ref in own[::4] for p in range(ref.shape[0])]
    rights = [ref[p] for ref in own[1::4] for p in range(ref.shape[0])]
    z = jnp.concatenate([ref[...] for ref in own[2::4]], axis=0)
    y = jnp.concatenate([ref[...] for ref in own[3::4]], axis=0)
    own_count = tile2.shape[0] // BLK
    pair_count = pairs_ref.shape[1] // own_count
    rows = BLK * own_count
    block, pair_at = place_ref[0], place_ref[1]
    row = iota((rows, rows), 0)
    col = iota((rows, rows), 1)
    same = (mod(row, own_count) == mod(col, own_count)).astype(F4)
    spread_row, spread_col = iota((LANE, rows), 0), iota((LANE, rows), 1)
    spread = onehot(spread_row == LIVE_AT + mod(spread_col, own_count))
    metas = [m[...] for m in (meta0, meta1, meta2)]
    masks = [same * mm(m, spread)[0:1, :] for m in metas]
    near_ref[...] = tile1a[...] + tile1b[...]
    tiles = [jnp.concatenate([t[...] for t in tile0], axis=0), near_ref, tile2]

    def spread_rows(value):
        return jnp.concatenate(
            [jnp.broadcast_to(value[p : p + 1], (own_count, rows)) for p in range(BLK)], axis=0
        )

    mixed = jnp.zeros((rows, PAIR), F4)
    for t in range(REACH + 1):
        pick = onehot(spread_row == (REACH + t) * BLK + div(spread_col, own_count))
        weight = spread_rows(mm(metas[0], pick)) * masks[t]
        mixed = mixed + mm(weight.astype(BF), tiles[t][...])
    mixed_ref[...] = mixed.astype(BF)
    other = jnp.zeros((rows, PAIR), F4)
    unspread = onehot(iota((BLK, rows), 0) == div(iota((BLK, rows), 1), own_count))
    for t in range(1, REACH + 1):
        pick = onehot(iota((BLK, LANE), 1) == (REACH - t) * BLK + iota((BLK, LANE), 0))
        weight = spread_rows(mm(mm_nt(pick, metas[t]).astype(BF), unspread)) * masks[t]
        other = other + mm(weight.astype(BF), tiles[t][...])
    other_ref[...] = other.astype(BF)
    selects = [
        onehot(slot_onehot(pair_row(pairs_ref, place_ref, s, own_count)))
        for s in range(pair_count)
    ]
    own_select = selects[0]
    both_parts = jnp.concatenate(selects, axis=1).astype(F4).T.astype(BF)
    both_parts = jnp.concatenate([both_parts, both_parts], axis=1)

    def chi_part(steps):
        crosses = []
        for t in steps:
            w = abs(t)
            if t < 0:
                crosses.append(mm_nt(tiles[w][...], y))
            else:
                crosses.append(mm_nt(z, tiles[w][...]))
        sums, picks = [], []
        for t, cross in zip(steps, crosses):
            cross = cross * masks[abs(t)]
            sums.append(
                jnp.concatenate(
                    [
                        jnp.sum(cross[p * own_count : (p + 1) * own_count], axis=0, keepdims=True)
                        for p in range(BLK)
                    ],
                    axis=0,
                )
            )
            picks.append(
                onehot(
                    iota((rows, LANE), 1)
                    == (REACH + t) * BLK + div(iota((rows, LANE), 0), own_count)
                )
            )
        return mm_split(jnp.concatenate(sums, axis=1), jnp.concatenate(picks, axis=0))

    parts = [
        mm(own_select, ref[r * own_count : (r + 1) * own_count]).astype(BF)
        for ref in (mixed_ref, other_ref)
        for r in range(BLK)
    ]
    values = [to_matrix(part) for part in parts]
    chi = chi_part((-2, 2)) + chi_part((-1, 1)) + chi_part((0,))
    scaled = mm(jnp.concatenate(values[:BLK], axis=0), cols_ref[...]).astype(BF)
    lefts = [scaled[r * NORB : (r + 1) * NORB] for r in range(BLK)]
    total = mm(jnp.concatenate(lefts, axis=1), jnp.concatenate(matrices, axis=0))
    total = total + mm(jnp.concatenate(rights, axis=1), jnp.concatenate(values[BLK:], axis=0))
    total = total * -sigma_scale
    high = total.astype(BF).astype(F4)
    parts = jnp.concatenate([from_matrix(high), from_matrix(total - high)], axis=0)
    owned_all = mm(both_parts, parts)
    parity = place_ref[2]
    half = own_count // 2
    for s in range(pair_count):
        owned = owned_all[s * own_count : (s + 1) * own_count]
        first, second = owned[:half], owned[half:]
        keep = jnp.where(parity == 0, first, second)
        send = jnp.where(parity == 0, second, first)
        for q in range(NQ):
            keep_ref[s, q * half : (q + 1) * half, :] = keep[:, q * LANE : (q + 1) * LANE]
            send_ref[s, q * half : (q + 1) * half, :] = send[:, q * LANE : (q + 1) * LANE]

    chi = chi * chi_scale
    share = (2 * REACH + 1) * BLK // pair_count
    column = iota((LANE, 1), 0)
    target = block + jnp.maximum(REACH - div(column, BLK), 0)
    at_pair = jnp.zeros((LANE, 1), jnp.int32)
    for s in range(1, pair_count):
        at_pair = at_pair + (column >= s * share).astype(jnp.int32)
    place = mod(at_pair - pair_at + pair_count, pair_count) + (
        ((target & 1) ^ place_ref[2]) * pair_count
    )
    spot = place * lanes + div(target, 2) * share + column - at_pair * share
    spread = onehot(iota((LANE, 2 * pair_count * lanes), 1) == spot)
    placed = mm_split(chi, spread)
    for s in range(pair_count):
        for i in range(lanes // LANE):
            at = slice(NQ * half + i * BLK, NQ * half + (i + 1) * BLK)
            begin = s * lanes + i * LANE
            keep_ref[s, at, :] = placed[:, begin : begin + LANE]
            begin += pair_count * lanes
            send_ref[s, at, :] = placed[:, begin : begin + LANE]


def last_kernel(place_ref, own_ref, other_ref, chi_ref, energy_ref):
    half = energy_ref.shape[0] // 2
    share = chi_ref.shape[1]
    parity = place_ref[2]
    own, other = own_ref[...], other_ref[...]
    first = jnp.where(parity == 0, own, other)
    second = jnp.where(parity == 0, other, own)
    for q in range(NQ):
        at = slice(q * LANE, (q + 1) * LANE)
        energy_ref[:half, at] = first[q * half : (q + 1) * half]
        energy_ref[half:, at] = second[q * half : (q + 1) * half]
    start = (place_ref[0] >> 1) * share
    total = None
    for i in range((own.shape[0] - NQ * half) // BLK):
        at = slice(NQ * half + i * BLK, NQ * half + (i + 1) * BLK)
        chi = jnp.where((place_ref[0] & 1) == parity, own[at], other[at])
        pick = onehot(iota((LANE, LANE), 0) + i * LANE == start + iota((LANE, LANE), 1))
        part = mm_split(chi, pick)
        total = part if total is None else total + part
    chi_ref[...] = total[:, :share]


def call(body, outs, *args, scratch=(), ins=None, flops=10**8):
    full = pl.BlockSpec(memory_space=pltpu.VMEM)
    ins = ins or full
    if ins is not full:
        args = [pltpu.with_memory_space_constraint(a, pltpu.HBM) for a in args]
    return pl.pallas_call(
        body,
        out_shape=outs,
        in_specs=[pl.BlockSpec(memory_space=pltpu.SMEM) if a.ndim == 1 else ins for a in args],
        out_specs=jax.tree.map(lambda o: full, outs),
        scratch_shapes=scratch,
        cost_estimate=pl.CostEstimate(flops=flops, bytes_accessed=10**6, transcendentals=0),
        compiler_params=pltpu.CompilerParams(vmem_limit_bytes=24 << 20),
    )(*args)


def per_device(three_center, tile_live, pair_atoms, green_occ, green_vir, screened):
    block_rows, own_count = three_center.shape[:2]
    aux_count, pair_count = lax.axis_size("aux"), lax.axis_size("pair")
    block, pair_at = lax.axis_index("aux"), lax.axis_index("pair")
    rows = block_rows * own_count
    window = screened.shape[1]
    shape = jax.ShapeDtypeStruct

    def shifted(value, steps, parity=None):
        return lax.ppermute(
            value,
            "aux",
            [
                (s, s + steps)
                for s in range(aux_count)
                if 0 <= s + steps < aux_count and parity in (None, s % 2)
            ],
        )

    def turned(value, steps):
        return lax.ppermute(
            value, "pair", [(s, (s - steps) % pair_count) for s in range(pair_count)]
        )

    def flipped(value, mask):
        return lax.ppermute(value, "aux", [(s, s ^ mask) for s in range(aux_count)])

    far = shifted(three_center, -2)
    near_even = shifted(three_center, -1, 1)
    square = shape((NORB, NORB), BF)
    pairs, vir, meta, both, cols, vir_t, *parts = call(
        tables_kernel,
        [
            shape((1, pair_count * own_count), jnp.int32),
            square,
            shape((block_rows, LANE), BF),
            shape((2 * NORB, NORB), BF),
            square,
            square,
        ]
        + [shape((c * own_count, PAIR), BF) for c in CHUNKS],
        green_occ,
        green_vir,
        screened,
        tile_live,
        pair_atoms.reshape(1, pair_count * own_count),
        three_center,
        scratch=[
            pltpu.VMEM((NORB, NORB), BF),
            pltpu.VMEM(screened.shape, BF),
            pltpu.VMEM(tile_live.shape, jnp.int32),
            pltpu.VMEM(three_center.shape, BF),
            pltpu.SemaphoreType.DMA((6,)),
        ],
        ins=pl.BlockSpec(memory_space=pltpu.HBM),
    )
    pieces = []
    for part in parts:
        pieces.append([part] + [turned(part, s) for s in range(1, pair_count)])
    meta_near = shifted(meta, -1)
    meta_far = shifted(meta, -2)
    near_odd = shifted(far, 1, 0)
    turn = pair_count == 2
    half_at = (lax.population_count(block) + (pair_at if turn else 0)) & 1
    place = jnp.stack([block, pair_at, half_at]).astype(jnp.int32)

    def joint(value, target):
        return lax.ppermute(
            value,
            ("aux", "pair"),
            [
                (s * pair_count + p, t * pair_count + q)
                for s in range(aux_count)
                for p in range(pair_count)
                for t, q in [target(s, p)]
            ],
        )

    own = []
    for c, count in enumerate(CHUNKS):
        own += call(
            lambda *refs: own_kernel(pair_count, own_count, *refs),
            [
                shape((count, NORB, NORB), BF),
                shape((count, NORB, NORB), BF),
                shape((count * own_count, PAIR), BF),
                shape((count * own_count, PAIR), BF),
            ],
            place,
            pairs,
            *pieces[c],
            both,
            cols,
            vir,
            vir_t,
        )

    lanes = -(-(aux_count // 2) * (window // pair_count) // LANE) * LANE
    message = shape((pair_count, own_count // 2 * NQ + lanes // LANE * BLK, LANE), F4)
    aux_total = block_rows * aux_count
    keep, send = call(
        lambda *refs: window_kernel(
            lanes, 1.0 / math.sqrt(aux_total * NAT * OA * NAT), 1.0 / (OA * NAT), *refs
        ),
        [message, message],
        place,
        pairs,
        meta,
        meta_near,
        meta_far,
        near_even.reshape(rows, PAIR),
        near_odd.reshape(rows, PAIR),
        far.reshape(rows, PAIR),
        cols,
        *own,
        *parts,
        scratch=[pltpu.VMEM((rows, PAIR), BF)] * 3,
    )
    total = keep + flipped(send, 1)
    owned = total[0]
    if turn:
        owned = owned + joint(total[1].astype(BF), lambda s, p: (s ^ 1, p ^ 1)).astype(F4)
    else:
        for s in range(1, pair_count):
            owned = owned + turned(total[s].astype(BF), -s).astype(F4)
    masks = [1 << i | 1 for i in range(1, (aux_count - 1).bit_length())]
    for masks_here in zip(masks, masks[1:] + masks[:1]):
        owned = owned + joint(
            owned,
            lambda s, p: (s ^ masks_here[(s.bit_count() + (p if turn else 0)) % 2], p),
        )
    polarizability, self_energy = call(
        last_kernel,
        [
            shape((block_rows, window // pair_count), F4),
            shape((own_count, PAIR), F4),
        ],
        place,
        owned,
        flipped(owned, 1),
    )
    return polarizability, self_energy


def solution(mesh):
    placed = (P("aux", "pair", None), P("aux", "pair"), P(), P(), P(), P("aux", None))
    return jax.shard_map(
        per_device,
        mesh=mesh,
        in_specs=placed,
        out_specs=(P("aux", "pair"), P("pair", None)),
        check_vma=False,
    )
```

```python
import math

import jax
import jax.numpy as jnp
from jax import lax
from jax.experimental import pallas as pl
from jax.experimental.pallas import tpu as pltpu
from jax.sharding import PartitionSpec as P


OA = 32
NAT = 8
REACH = 2
BLK = 8
NORB = OA * NAT
PAIR = OA * OA
LANE = 128
RQ = LANE // OA
NQ = OA // RQ
LIVE_AT = 64
CHUNKS = (4, 4)
BF = jnp.bfloat16
F4 = jnp.float32


def iota(shape, dim):
    return lax.broadcasted_iota(jnp.int32, shape, dim)


def mm(a, b):
    return lax.dot_general(a, b, (((1,), (0,)), ((), ())), preferred_element_type=F4)


def mm_nt(a, b):
    return lax.dot_general(a, b, (((1,), (1,)), ((), ())), preferred_element_type=F4)


def onehot(cond):
    return cond.astype(F4).astype(BF)


def div(x, n):
    if n & (n - 1) == 0:
        return lax.shift_right_logical(x, jnp.full_like(x, n.bit_length() - 1))
    return x // n


def mod(x, n):
    if n & (n - 1) == 0:
        return x & (n - 1)
    return x % n


def mm_split(a, b):
    count = a.shape[0]
    high = a.astype(BF)
    rest = a - high.astype(F4)
    middle = rest.astype(BF)
    low = (rest - middle.astype(F4)).astype(BF)
    out = mm(jnp.concatenate([high.astype(F4), middle.astype(F4), low.astype(F4)], axis=0).astype(BF), b)
    return out[:count] + out[count : 2 * count] + out[2 * count :]


def slot_onehot(pair_row):
    count = pair_row.shape[1]
    slot = iota((NAT * NAT, count), 0)
    second = mod(div(slot, NAT), 2) * RQ + div(slot, 2 * NAT)
    return mod(slot, NAT) * NAT + second == pair_row


def pair_row(pairs_ref, place_ref, step, own_count):
    count = pairs_ref.shape[1] // own_count
    at = mod(place_ref[1] + step, count)
    row = jnp.zeros((1, own_count), jnp.int32)
    for s in range(count):
        row = jnp.where(at == s, pairs_ref[0:1, s * own_count : (s + 1) * own_count], row)
    return row


def swap_blocks(parts):
    lane = iota(parts[0].shape, 1)
    low = lane < LANE // 2
    even = mod(lane, LANE // 2) < OA
    a, b, c, d = parts
    moved = pltpu.roll(jnp.where(low, c, a), LANE // 2, 1)
    a, c = jnp.where(low, a, moved), jnp.where(low, moved, c)
    moved = pltpu.roll(jnp.where(low, d, b), LANE // 2, 1)
    b, d = jnp.where(low, b, moved), jnp.where(low, moved, d)
    a, b = jnp.where(even, a, pltpu.roll(b, OA, 1)), jnp.where(even, pltpu.roll(a, LANE - OA, 1), b)
    c, d = jnp.where(even, c, pltpu.roll(d, OA, 1)), jnp.where(even, pltpu.roll(c, LANE - OA, 1), d)
    return a, b, c, d


def to_matrix(tiles):
    parts = [
        jnp.concatenate(
            [tiles[i * 2 * NAT : (i + 1) * 2 * NAT, q * LANE : (q + 1) * LANE] for q in range(NQ)],
            axis=0,
        )
        for i in range(RQ)
    ]
    parts = [part.astype(F4) for part in swap_blocks(parts)]
    out = [
        jnp.concatenate(
            [part[(q * 2 + g) * NAT : (q * 2 + g + 1) * NAT] for g in range(2)], axis=1
        )
        for part in parts
        for q in range(NQ)
    ]
    return jnp.concatenate(out, axis=0).astype(BF)


def from_matrix(matrix):
    parts = [
        jnp.concatenate(
            [
                matrix[(i * NQ + q) * NAT : (i * NQ + q + 1) * NAT, g * LANE : (g + 1) * LANE]
                for q in range(NQ)
                for g in range(2)
            ],
            axis=0,
        ).astype(BF)
        for i in range(RQ)
    ]
    return jnp.concatenate(
        [
            jnp.concatenate(
                [part[q * 2 * NAT : (q + 1) * 2 * NAT] for q in range(NQ)], axis=1
            )
            for part in swap_blocks(parts)
        ],
        axis=0,
    )


def load(ins, targets, sems):
    copies = [
        pltpu.make_async_copy(a, b, sems.at[i]) for i, (a, b) in enumerate(zip(ins, targets))
    ]
    for copy in copies:
        copy.start()
    return copies


def mask_rows(ref, live_row, whole_ref):
    own_count = live_row.shape[1]
    diagonal = iota((own_count, own_count), 0) == iota((own_count, own_count), 1)
    live = jnp.sum(jnp.where(diagonal, live_row.astype(F4), 0.0), axis=1, keepdims=True).astype(BF)
    for p in range(whole_ref.shape[0]):
        ref[p * own_count : (p + 1) * own_count] = whole_ref[p] * live


def pack_kernel(live_hbm, whole_hbm, part_ref, live_ref, whole_ref, sems):
    copies = load((live_hbm, whole_hbm.at[: CHUNKS[0]]), (live_ref, whole_ref), sems)
    for copy in copies:
        copy.wait()
    mask_rows(part_ref, live_ref[...], whole_ref)


def tables_kernel(*refs):
    ins, outs = refs[:6], refs[6:-5]
    pairs_ref, vir_ref, meta_ref, both_ref, cols_ref, vir_t_ref, part_ref = outs
    occ_ref, screened_ref, live_ref, whole_ref, sems = refs[-5:]
    targets = (occ_ref, vir_ref, screened_ref, live_ref, pairs_ref, whole_ref)
    copies = load(ins[:-1] + (ins[-1].at[CHUNKS[0] :],), targets, sems)
    for copy in copies[:-1]:
        copy.wait()
    own_count = live_ref.shape[1]
    meta_ref[...] = jnp.zeros(meta_ref.shape, BF)
    meta_ref[:, : screened_ref.shape[1]] = screened_ref[...]
    meta_ref[:, LIVE_AT : LIVE_AT + own_count] = jnp.broadcast_to(
        live_ref[...].astype(F4), (BLK, own_count)
    ).astype(BF)
    row = iota((NORB, NORB), 0)
    col = iota((NORB, NORB), 1)
    natural = mod(row, NAT) * OA + mod(div(row, NAT), NQ) * RQ + div(row, NAT * NQ)
    order = onehot(natural == col)
    occ = occ_ref[...]
    cols = mm_nt(occ, order).astype(BF)
    both = mm(order, cols)
    cols_ref[...] = cols
    both_ref[:NORB] = both.T.astype(BF)
    both_ref[NORB:] = both.astype(BF)
    vir_t_ref[...] = vir_ref[...].astype(F4).T.astype(BF)
    copies[-1].wait()
    mask_rows(part_ref, live_ref[...], whole_ref)


def own_kernel(count, own_count, place_ref, pairs_ref, *refs):
    pieces = refs[:count]
    both_ref, cols_ref, vir_ref, vir_t_ref = refs[count : count + 4]
    matrix_ref, right_ref, z_ref, y_ref = refs[count + 4 :]
    group = matrix_ref.shape[0]
    selects = [
        onehot(slot_onehot(pair_row(pairs_ref, place_ref, s, own_count))) for s in range(count)
    ]
    tiles = []
    for p in range(group):
        at = slice(p * own_count, (p + 1) * own_count)
        total = mm(selects[0], pieces[0][at])
        for s in range(1, count):
            total = total + mm(selects[s], pieces[s][at])
        tiles.append(total.astype(BF))
    own_select = slot_onehot(pair_row(pairs_ref, place_ref, 0, own_count)).astype(F4).T.astype(BF)
    matrices = [to_matrix(t) for t in tiles]
    both = both_ref[...]

    def transformed(rows, side):
        lefts = [mm(both[rows], m).astype(BF) for m in matrices]
        value = mm(jnp.concatenate(lefts, axis=0), side)
        return [value[p * NORB : (p + 1) * NORB] for p in range(group)]

    def selected(value, ref):
        for p in range(group):
            part = from_matrix(value[p])
            ref[p * own_count : (p + 1) * own_count] = mm(own_select, part).astype(BF)

    z = transformed(slice(0, NORB), vir_ref[...])
    y = transformed(slice(NORB, 2 * NORB), vir_t_ref[...])
    selected(z, z_ref)
    right = mm(jnp.concatenate(matrices, axis=0), cols_ref[...]).astype(BF)
    for p in range(group):
        matrix_ref[p] = matrices[p]
        right_ref[p] = right[p * NORB : (p + 1) * NORB]
    selected(y, y_ref)


def window_kernel(lanes, sigma_scale, chi_scale, place_ref, *refs):
    (pairs_ref, meta0, meta1a, meta1b, meta2, tile1a, tile1b, tile2, cols_ref) = refs[:9]
    keep_ref, send_ref, near_ref, mixed_ref, other_ref = refs[-5:]
    own, tile0 = refs[9 : 9 + 4 * len(CHUNKS)], refs[9 + 4 * len(CHUNKS) : -5]
    matrices = [ref[p] for ref in own[::4] for p in range(ref.shape[0])]
    rights = [ref[p] for ref in own[1::4] for p in range(ref.shape[0])]
    z = jnp.concatenate([ref[...] for ref in own[2::4]], axis=0)
    y = jnp.concatenate([ref[...] for ref in own[3::4]], axis=0)
    own_count = tile2.shape[0] // BLK
    pair_count = pairs_ref.shape[1] // own_count
    rows = BLK * own_count
    block, pair_at = place_ref[0], place_ref[1]
    row = iota((rows, rows), 0)
    col = iota((rows, rows), 1)
    same = (mod(row, own_count) == mod(col, own_count)).astype(F4)
    spread_row, spread_col = iota((LANE, rows), 0), iota((LANE, rows), 1)
    spread = onehot(spread_row == LIVE_AT + mod(spread_col, own_count))
    metas = [meta0[...], jnp.where((block & 1) == 0, meta1a[...], meta1b[...]), meta2[...]]
    masks = [same * mm(m, spread)[0:1, :] for m in metas]
    near_ref[...] = jnp.where((block & 1) == 0, tile1a[...], tile1b[...])
    tiles = [jnp.concatenate([t[...] for t in tile0], axis=0), near_ref, tile2]

    def spread_rows(value):
        return jnp.concatenate(
            [jnp.broadcast_to(value[p : p + 1], (own_count, rows)) for p in range(BLK)], axis=0
        )

    mixed = jnp.zeros((rows, PAIR), F4)
    for t in range(REACH + 1):
        pick = onehot(spread_row == (REACH + t) * BLK + div(spread_col, own_count))
        weight = spread_rows(mm(metas[0], pick)) * masks[t]
        mixed = mixed + mm(weight.astype(BF), tiles[t][...])
    mixed_ref[...] = mixed.astype(BF)
    other = jnp.zeros((rows, PAIR), F4)
    unspread = onehot(iota((BLK, rows), 0) == div(iota((BLK, rows), 1), own_count))
    for t in range(1, REACH + 1):
        pick = onehot(iota((BLK, LANE), 1) == (REACH - t) * BLK + iota((BLK, LANE), 0))
        weight = spread_rows(mm(mm_nt(pick, metas[t]).astype(BF), unspread)) * masks[t]
        other = other + mm(weight.astype(BF), tiles[t][...])
    other_ref[...] = other.astype(BF)
    selects = [
        onehot(slot_onehot(pair_row(pairs_ref, place_ref, s, own_count)))
        for s in range(pair_count)
    ]
    own_select = selects[0]
    both_parts = jnp.concatenate(selects, axis=1).astype(F4).T.astype(BF)
    both_parts = jnp.concatenate([both_parts, both_parts], axis=1)

    def chi_part(steps):
        crosses = []
        for t in steps:
            w = abs(t)
            if t < 0:
                crosses.append(mm_nt(tiles[w][...], y))
            else:
                crosses.append(mm_nt(z, tiles[w][...]))
        sums, picks = [], []
        for t, cross in zip(steps, crosses):
            cross = cross * masks[abs(t)]
            sums.append(
                jnp.concatenate(
                    [
                        jnp.sum(cross[p * own_count : (p + 1) * own_count], axis=0, keepdims=True)
                        for p in range(BLK)
                    ],
                    axis=0,
                )
            )
            picks.append(
                onehot(
                    iota((rows, LANE), 1)
                    == (REACH + t) * BLK + div(iota((rows, LANE), 0), own_count)
                )
            )
        return mm_split(jnp.concatenate(sums, axis=1), jnp.concatenate(picks, axis=0))

    parts = [
        mm(own_select, ref[r * own_count : (r + 1) * own_count]).astype(BF)
        for ref in (mixed_ref, other_ref)
        for r in range(BLK)
    ]
    values = [to_matrix(part) for part in parts]
    chi = chi_part((-2, 2)) + chi_part((-1, 1)) + chi_part((0,))
    scaled = mm(jnp.concatenate(values[:BLK], axis=0), cols_ref[...]).astype(BF)
    lefts = [scaled[r * NORB : (r + 1) * NORB] for r in range(BLK)]
    total = mm(jnp.concatenate(lefts, axis=1), jnp.concatenate(matrices, axis=0))
    total = total + mm(jnp.concatenate(rights, axis=1), jnp.concatenate(values[BLK:], axis=0))
    total = total * -sigma_scale
    high = total.astype(BF).astype(F4)
    parts = jnp.concatenate([from_matrix(high), from_matrix(total - high)], axis=0)
    owned_all = mm(both_parts, parts)
    parity = place_ref[2]
    half = own_count // 2
    for s in range(pair_count):
        owned = owned_all[s * own_count : (s + 1) * own_count]
        first, second = owned[:half], owned[half:]
        keep = jnp.where(parity == 0, first, second)
        send = jnp.where(parity == 0, second, first)
        for q in range(NQ):
            keep_ref[s, q * half : (q + 1) * half, :] = keep[:, q * LANE : (q + 1) * LANE]
            send_ref[s, q * half : (q + 1) * half, :] = send[:, q * LANE : (q + 1) * LANE]

    chi = chi * chi_scale
    share = (2 * REACH + 1) * BLK // pair_count
    column = iota((LANE, 1), 0)
    target = block + jnp.maximum(REACH - div(column, BLK), 0)
    at_pair = jnp.zeros((LANE, 1), jnp.int32)
    for s in range(1, pair_count):
        at_pair = at_pair + (column >= s * share).astype(jnp.int32)
    place = mod(at_pair - pair_at + pair_count, pair_count) + (
        ((target & 1) ^ place_ref[2]) * pair_count
    )
    spot = place * lanes + div(target, 2) * share + column - at_pair * share
    spread = onehot(iota((LANE, 2 * pair_count * lanes), 1) == spot)
    placed = mm_split(chi, spread)
    for s in range(pair_count):
        for i in range(lanes // LANE):
            at = slice(NQ * half + i * BLK, NQ * half + (i + 1) * BLK)
            begin = s * lanes + i * LANE
            keep_ref[s, at, :] = placed[:, begin : begin + LANE]
            begin += pair_count * lanes
            send_ref[s, at, :] = placed[:, begin : begin + LANE]


def last_kernel(place_ref, own_ref, other_ref, chi_ref, energy_ref):
    half = energy_ref.shape[0] // 2
    share = chi_ref.shape[1]
    parity = place_ref[2]
    own, other = own_ref[...], other_ref[...]
    first = jnp.where(parity == 0, own, other)
    second = jnp.where(parity == 0, other, own)
    for q in range(NQ):
        at = slice(q * LANE, (q + 1) * LANE)
        energy_ref[:half, at] = first[q * half : (q + 1) * half]
        energy_ref[half:, at] = second[q * half : (q + 1) * half]
    start = (place_ref[0] >> 1) * share
    total = None
    for i in range((own.shape[0] - NQ * half) // BLK):
        at = slice(NQ * half + i * BLK, NQ * half + (i + 1) * BLK)
        chi = jnp.where((place_ref[0] & 1) == parity, own[at], other[at])
        pick = onehot(iota((LANE, LANE), 0) + i * LANE == start + iota((LANE, LANE), 1))
        part = mm_split(chi, pick)
        total = part if total is None else total + part
    chi_ref[...] = total[:, :share]


def call(body, outs, *args, scratch=(), ins=None, flops=10**8):
    full = pl.BlockSpec(memory_space=pltpu.VMEM)
    ins = ins or full
    if ins is not full:
        args = [pltpu.with_memory_space_constraint(a, pltpu.HBM) for a in args]
    return pl.pallas_call(
        body,
        out_shape=outs,
        in_specs=[pl.BlockSpec(memory_space=pltpu.SMEM) if a.ndim == 1 else ins for a in args],
        out_specs=jax.tree.map(lambda o: full, outs),
        scratch_shapes=scratch,
        cost_estimate=pl.CostEstimate(flops=flops, bytes_accessed=10**6, transcendentals=0),
        compiler_params=pltpu.CompilerParams(vmem_limit_bytes=24 << 20),
    )(*args)


def per_device(three_center, tile_live, pair_atoms, green_occ, green_vir, screened):
    block_rows, own_count = three_center.shape[:2]
    aux_count, pair_count = lax.axis_size("aux"), lax.axis_size("pair")
    block, pair_at = lax.axis_index("aux"), lax.axis_index("pair")
    rows = block_rows * own_count
    window = screened.shape[1]
    shape = jax.ShapeDtypeStruct

    def shifted(value, steps, parity=None):
        return lax.ppermute(
            value,
            "aux",
            [
                (s, s + steps)
                for s in range(aux_count)
                if 0 <= s + steps < aux_count and parity in (None, s % 2)
            ],
        )

    def turned(value, steps):
        return lax.ppermute(
            value, "pair", [(s, (s - steps) % pair_count) for s in range(pair_count)]
        )

    def flipped(value, mask):
        return lax.ppermute(value, "aux", [(s, s ^ mask) for s in range(aux_count)])

    far = shifted(three_center, -2)
    near_even = flipped(three_center, 1)
    square = shape((NORB, NORB), BF)

    def part_of(c):
        return shape((CHUNKS[c] * own_count, PAIR), BF)

    def whole_of(c):
        return pltpu.VMEM((CHUNKS[c], own_count, PAIR), BF)

    hbm = pl.BlockSpec(memory_space=pltpu.HBM)
    first_part = call(
        pack_kernel,
        [part_of(0)],
        tile_live,
        three_center,
        scratch=[
            pltpu.VMEM(tile_live.shape, jnp.int32),
            whole_of(0),
            pltpu.SemaphoreType.DMA((2,)),
        ],
        ins=hbm,
    )[0]
    pairs, vir, meta, both, cols, vir_t, second_part = call(
        tables_kernel,
        [
            shape((1, pair_count * own_count), jnp.int32),
            square,
            shape((block_rows, LANE), BF),
            shape((2 * NORB, NORB), BF),
            square,
            square,
            part_of(1),
        ],
        green_occ,
        green_vir,
        screened,
        tile_live,
        pair_atoms.reshape(1, pair_count * own_count),
        three_center,
        scratch=[
            pltpu.VMEM((NORB, NORB), BF),
            pltpu.VMEM(screened.shape, BF),
            pltpu.VMEM(tile_live.shape, jnp.int32),
            whole_of(1),
            pltpu.SemaphoreType.DMA((6,)),
        ],
        ins=hbm,
    )
    parts = [first_part, second_part]
    pieces = []
    for part in parts:
        pieces.append([part] + [turned(part, s) for s in range(1, pair_count)])
    meta_even = flipped(meta, 1)
    meta_far = shifted(meta, -2)
    near_odd = flipped(far, 1)
    meta_odd = flipped(meta_far, 1)
    turn = pair_count == 2
    half_at = (lax.population_count(block) + (pair_at if turn else 0)) & 1
    place = jnp.stack([block, pair_at, half_at]).astype(jnp.int32)

    def joint(value, target):
        return lax.ppermute(
            value,
            ("aux", "pair"),
            [
                (s * pair_count + p, t * pair_count + q)
                for s in range(aux_count)
                for p in range(pair_count)
                for t, q in [target(s, p)]
            ],
        )

    own = []
    for c, count in enumerate(CHUNKS):
        own += call(
            lambda *refs: own_kernel(pair_count, own_count, *refs),
            [
                shape((count, NORB, NORB), BF),
                shape((count, NORB, NORB), BF),
                shape((count * own_count, PAIR), BF),
                shape((count * own_count, PAIR), BF),
            ],
            place,
            pairs,
            *pieces[c],
            both,
            cols,
            vir,
            vir_t,
        )

    lanes = -(-(aux_count // 2) * (window // pair_count) // LANE) * LANE
    message = shape((pair_count, own_count // 2 * NQ + lanes // LANE * BLK, LANE), F4)
    aux_total = block_rows * aux_count
    keep, send = call(
        lambda *refs: window_kernel(
            lanes, 1.0 / math.sqrt(aux_total * NAT * OA * NAT), 1.0 / (OA * NAT), *refs
        ),
        [message, message],
        place,
        pairs,
        meta,
        meta_even,
        meta_odd,
        meta_far,
        near_even.reshape(rows, PAIR),
        near_odd.reshape(rows, PAIR),
        far.reshape(rows, PAIR),
        cols,
        *own,
        *parts,
        scratch=[pltpu.VMEM((rows, PAIR), BF)] * 3,
    )
    total = keep + flipped(send, 1)
    owned = total[0]
    if turn:
        owned = owned + joint(total[1].astype(BF), lambda s, p: (s ^ 1, p ^ 1)).astype(F4)
    else:
        for s in range(1, pair_count):
            owned = owned + turned(total[s].astype(BF), -s).astype(F4)
    masks = [1 << i | 1 for i in range(1, (aux_count - 1).bit_length())]
    for masks_here in zip(masks, masks[1:] + masks[:1]):
        owned = owned + joint(
            owned,
            lambda s, p: (s ^ masks_here[(s.bit_count() + (p if turn else 0)) % 2], p),
        )
    polarizability, self_energy = call(
        last_kernel,
        [
            shape((block_rows, window // pair_count), F4),
            shape((own_count, PAIR), F4),
        ],
        place,
        owned,
        flipped(owned, 1),
    )
    return polarizability, self_energy


def solution(mesh):
    placed = (P("aux", "pair", None), P("aux", "pair"), P(), P(), P(), P("aux", None))
    return jax.shard_map(
        per_device,
        mesh=mesh,
        in_specs=placed,
        out_specs=(P("aux", "pair"), P("pair", None)),
        check_vma=False,
    )
```

```python
import math

import jax
import jax.numpy as jnp
from jax import lax
from jax.experimental import pallas as pl
from jax.experimental.pallas import tpu as pltpu
from jax.sharding import PartitionSpec as P


OA = 32
NAT = 8
REACH = 2
BLK = 8
NORB = OA * NAT
PAIR = OA * OA
LANE = 128
RQ = LANE // OA
NQ = OA // RQ
LIVE_AT = 64
CHUNKS = (5, 3)
BF = jnp.bfloat16
F4 = jnp.float32


def iota(shape, dim):
    return lax.broadcasted_iota(jnp.int32, shape, dim)


def mm(a, b):
    return lax.dot_general(a, b, (((1,), (0,)), ((), ())), preferred_element_type=F4)


def mm_nt(a, b):
    return lax.dot_general(a, b, (((1,), (1,)), ((), ())), preferred_element_type=F4)


def onehot(cond):
    return cond.astype(F4).astype(BF)


def div(x, n):
    if n & (n - 1) == 0:
        return lax.shift_right_logical(x, jnp.full_like(x, n.bit_length() - 1))
    return x // n


def mod(x, n):
    if n & (n - 1) == 0:
        return x & (n - 1)
    return x % n


def mm_split(a, b):
    count = a.shape[0]
    high = a.astype(BF)
    rest = a - high.astype(F4)
    middle = rest.astype(BF)
    low = (rest - middle.astype(F4)).astype(BF)
    out = mm(jnp.concatenate([high.astype(F4), middle.astype(F4), low.astype(F4)], axis=0).astype(BF), b)
    return out[:count] + out[count : 2 * count] + out[2 * count :]


def slot_onehot(pair_row):
    count = pair_row.shape[1]
    slot = iota((NAT * NAT, count), 0)
    second = mod(div(slot, NAT), 2) * RQ + div(slot, 2 * NAT)
    return mod(slot, NAT) * NAT + second == pair_row


def pair_row(pairs_ref, place_ref, step, own_count):
    count = pairs_ref.shape[1] // own_count
    at = mod(place_ref[1] + step, count)
    row = jnp.zeros((1, own_count), jnp.int32)
    for s in range(count):
        row = jnp.where(at == s, pairs_ref[0:1, s * own_count : (s + 1) * own_count], row)
    return row


def swap_blocks(parts):
    lane = iota(parts[0].shape, 1)
    low = lane < LANE // 2
    even = mod(lane, LANE // 2) < OA
    a, b, c, d = parts
    moved = pltpu.roll(jnp.where(low, c, a), LANE // 2, 1)
    a, c = jnp.where(low, a, moved), jnp.where(low, moved, c)
    moved = pltpu.roll(jnp.where(low, d, b), LANE // 2, 1)
    b, d = jnp.where(low, b, moved), jnp.where(low, moved, d)
    a, b = jnp.where(even, a, pltpu.roll(b, OA, 1)), jnp.where(even, pltpu.roll(a, LANE - OA, 1), b)
    c, d = jnp.where(even, c, pltpu.roll(d, OA, 1)), jnp.where(even, pltpu.roll(c, LANE - OA, 1), d)
    return a, b, c, d


def to_matrix(tiles):
    parts = [
        jnp.concatenate(
            [tiles[i * 2 * NAT : (i + 1) * 2 * NAT, q * LANE : (q + 1) * LANE] for q in range(NQ)],
            axis=0,
        )
        for i in range(RQ)
    ]
    parts = [part.astype(F4) for part in swap_blocks(parts)]
    out = [
        jnp.concatenate(
            [part[(q * 2 + g) * NAT : (q * 2 + g + 1) * NAT] for g in range(2)], axis=1
        )
        for part in parts
        for q in range(NQ)
    ]
    return jnp.concatenate(out, axis=0).astype(BF)


def from_matrix(matrix):
    parts = [
        jnp.concatenate(
            [
                matrix[(i * NQ + q) * NAT : (i * NQ + q + 1) * NAT, g * LANE : (g + 1) * LANE]
                for q in range(NQ)
                for g in range(2)
            ],
            axis=0,
        ).astype(BF)
        for i in range(RQ)
    ]
    return jnp.concatenate(
        [
            jnp.concatenate(
                [part[q * 2 * NAT : (q + 1) * 2 * NAT] for q in range(NQ)], axis=1
            )
            for part in swap_blocks(parts)
        ],
        axis=0,
    )


def load(ins, targets, sems):
    copies = [
        pltpu.make_async_copy(a, b, sems.at[i]) for i, (a, b) in enumerate(zip(ins, targets))
    ]
    for copy in copies:
        copy.start()
    return copies


def mask_rows(ref, live_row, whole_ref):
    own_count = live_row.shape[1]
    diagonal = iota((own_count, own_count), 0) == iota((own_count, own_count), 1)
    live = jnp.sum(jnp.where(diagonal, live_row.astype(F4), 0.0), axis=1, keepdims=True).astype(BF)
    for p in range(whole_ref.shape[0]):
        ref[p * own_count : (p + 1) * own_count] = whole_ref[p] * live


def pack_kernel(live_hbm, whole_hbm, part_ref, live_ref, whole_ref, sems):
    copies = load((live_hbm, whole_hbm.at[: CHUNKS[0]]), (live_ref, whole_ref), sems)
    for copy in copies:
        copy.wait()
    mask_rows(part_ref, live_ref[...], whole_ref)


def tables_kernel(*refs):
    ins, outs = refs[:6], refs[6:-5]
    pairs_ref, vir_ref, meta_ref, both_ref, cols_ref, vir_t_ref, part_ref = outs
    occ_ref, screened_ref, live_ref, whole_ref, sems = refs[-5:]
    targets = (occ_ref, vir_ref, screened_ref, live_ref, pairs_ref, whole_ref)
    copies = load(ins[:-1] + (ins[-1].at[CHUNKS[0] :],), targets, sems)
    for copy in copies[:-1]:
        copy.wait()
    own_count = live_ref.shape[1]
    meta_ref[...] = jnp.zeros(meta_ref.shape, BF)
    meta_ref[:, : screened_ref.shape[1]] = screened_ref[...]
    meta_ref[:, LIVE_AT : LIVE_AT + own_count] = jnp.broadcast_to(
        live_ref[...].astype(F4), (BLK, own_count)
    ).astype(BF)
    row = iota((NORB, NORB), 0)
    col = iota((NORB, NORB), 1)
    natural = mod(row, NAT) * OA + mod(div(row, NAT), NQ) * RQ + div(row, NAT * NQ)
    order = onehot(natural == col)
    occ = occ_ref[...]
    cols = mm_nt(occ, order).astype(BF)
    both = mm(order, cols)
    cols_ref[...] = cols
    both_ref[:NORB] = both.T.astype(BF)
    both_ref[NORB:] = both.astype(BF)
    vir_t_ref[...] = vir_ref[...].astype(F4).T.astype(BF)
    copies[-1].wait()
    mask_rows(part_ref, live_ref[...], whole_ref)


def own_kernel(count, own_count, place_ref, pairs_ref, *refs):
    pieces = refs[:count]
    both_ref, cols_ref, vir_ref, vir_t_ref = refs[count : count + 4]
    matrix_ref, right_ref, z_ref, y_ref = refs[count + 4 :]
    group = matrix_ref.shape[0]
    selects = [
        onehot(slot_onehot(pair_row(pairs_ref, place_ref, s, own_count))) for s in range(count)
    ]
    tiles = []
    for p in range(group):
        at = slice(p * own_count, (p + 1) * own_count)
        total = mm(selects[0], pieces[0][at])
        for s in range(1, count):
            total = total + mm(selects[s], pieces[s][at])
        tiles.append(total.astype(BF))
    own_select = slot_onehot(pair_row(pairs_ref, place_ref, 0, own_count)).astype(F4).T.astype(BF)
    matrices = [to_matrix(t) for t in tiles]
    both = both_ref[...]

    def transformed(rows, side):
        lefts = [mm(both[rows], m).astype(BF) for m in matrices]
        value = mm(jnp.concatenate(lefts, axis=0), side)
        return [value[p * NORB : (p + 1) * NORB] for p in range(group)]

    def selected(value, ref):
        for p in range(group):
            part = from_matrix(value[p])
            ref[p * own_count : (p + 1) * own_count] = mm(own_select, part).astype(BF)

    z = transformed(slice(0, NORB), vir_ref[...])
    y = transformed(slice(NORB, 2 * NORB), vir_t_ref[...])
    selected(z, z_ref)
    right = mm(jnp.concatenate(matrices, axis=0), cols_ref[...]).astype(BF)
    for p in range(group):
        matrix_ref[p] = matrices[p]
        right_ref[p] = right[p * NORB : (p + 1) * NORB]
    selected(y, y_ref)


def spread_rows(value, own_count):
    return jnp.concatenate(
        [jnp.broadcast_to(value[p : p + 1], (own_count, value.shape[1])) for p in range(BLK)],
        axis=0,
    )


def early_kernel(meta_ref, *refs):
    parts, (base_ref, weight_ref) = refs[:-2], refs[-2:]
    rows = base_ref.shape[0]
    own_count = rows // BLK
    row, col = iota((rows, rows), 0), iota((rows, rows), 1)
    same = (mod(row, own_count) == mod(col, own_count)).astype(F4)
    spread_row, spread_col = iota((LANE, rows), 0), iota((LANE, rows), 1)
    meta = meta_ref[...]
    for t in range(REACH + 1):
        pick = onehot(spread_row == (REACH + t) * BLK + div(spread_col, own_count))
        weight = (spread_rows(mm(meta, pick), own_count) * same).astype(BF)
        if t:
            weight_ref[(t - 1) * rows : t * rows] = weight
        else:
            base_ref[...] = mm(weight, jnp.concatenate([p[...] for p in parts], axis=0))


def window_kernel(lanes, sigma_scale, chi_scale, place_ref, *refs):
    (pairs_ref, meta1a, meta1b, meta2, tile1a, tile1b, tile2, cols_ref) = refs[:8]
    base_ref, weight_ref = refs[8:10]
    keep_ref, send_ref, near_ref, mixed_ref, other_ref = refs[-5:]
    own, tile0 = refs[10 : 10 + 4 * len(CHUNKS)], refs[10 + 4 * len(CHUNKS) : -5]
    matrices = [ref[p] for ref in own[::4] for p in range(ref.shape[0])]
    rights = [ref[p] for ref in own[1::4] for p in range(ref.shape[0])]
    z = jnp.concatenate([ref[...] for ref in own[2::4]], axis=0)
    y = jnp.concatenate([ref[...] for ref in own[3::4]], axis=0)
    own_count = tile2.shape[0] // BLK
    pair_count = pairs_ref.shape[1] // own_count
    rows = BLK * own_count
    block, pair_at = place_ref[0], place_ref[1]
    metas = [None, jnp.where((block & 1) == 0, meta1a[...], meta1b[...]), meta2[...]]
    spread = onehot(iota((LANE, rows), 0) == LIVE_AT + mod(iota((LANE, rows), 1), own_count))
    lives = [None] + [mm(m, spread)[0:1, :] for m in metas[1:]]
    row, col = iota((rows, rows), 0), iota((rows, rows), 1)
    same = (mod(row, own_count) == mod(col, own_count)).astype(F4)
    masks = [same] + [same * live for live in lives[1:]]
    near_ref[...] = jnp.where((block & 1) == 0, tile1a[...], tile1b[...])
    tiles = [jnp.concatenate([t[...] for t in tile0], axis=0), near_ref, tile2]
    mixed = base_ref[...]
    for t in range(1, REACH + 1):
        weight = weight_ref[(t - 1) * rows : t * rows].astype(F4) * lives[t]
        mixed = mixed + mm(weight.astype(BF), tiles[t][...])
    mixed_ref[...] = mixed.astype(BF)
    other = jnp.zeros((rows, PAIR), F4)
    unspread = onehot(iota((BLK, rows), 0) == div(iota((BLK, rows), 1), own_count))
    for t in range(1, REACH + 1):
        pick = onehot(iota((BLK, LANE), 1) == (REACH - t) * BLK + iota((BLK, LANE), 0))
        weight = spread_rows(mm(mm_nt(pick, metas[t]).astype(BF), unspread), own_count) * masks[t]
        other = other + mm(weight.astype(BF), tiles[t][...])
    other_ref[...] = other.astype(BF)
    selects = [
        onehot(slot_onehot(pair_row(pairs_ref, place_ref, s, own_count)))
        for s in range(pair_count)
    ]
    own_select = selects[0]
    both_parts = jnp.concatenate(selects, axis=1).astype(F4).T.astype(BF)
    both_parts = jnp.concatenate([both_parts, both_parts], axis=1)

    def chi_part(steps):
        crosses = []
        for t in steps:
            w = abs(t)
            if t < 0:
                crosses.append(mm_nt(tiles[w][...], y))
            else:
                crosses.append(mm_nt(z, tiles[w][...]))
        sums, picks = [], []
        for t, cross in zip(steps, crosses):
            cross = cross * masks[abs(t)]
            sums.append(
                jnp.concatenate(
                    [
                        jnp.sum(cross[p * own_count : (p + 1) * own_count], axis=0, keepdims=True)
                        for p in range(BLK)
                    ],
                    axis=0,
                )
            )
            picks.append(
                onehot(
                    iota((rows, LANE), 1)
                    == (REACH + t) * BLK + div(iota((rows, LANE), 0), own_count)
                )
            )
        return mm_split(jnp.concatenate(sums, axis=1), jnp.concatenate(picks, axis=0))

    parts = [
        mm(own_select, ref[r * own_count : (r + 1) * own_count]).astype(BF)
        for ref in (mixed_ref, other_ref)
        for r in range(BLK)
    ]
    values = [to_matrix(part) for part in parts]
    chi = chi_part((-2, 2)) + chi_part((-1, 1)) + chi_part((0,))
    scaled = mm(jnp.concatenate(values[:BLK], axis=0), cols_ref[...]).astype(BF)
    lefts = [scaled[r * NORB : (r + 1) * NORB] for r in range(BLK)]
    total = mm(jnp.concatenate(lefts, axis=1), jnp.concatenate(matrices, axis=0))
    total = total + mm(jnp.concatenate(rights, axis=1), jnp.concatenate(values[BLK:], axis=0))
    total = total * -sigma_scale
    high = total.astype(BF).astype(F4)
    parts = jnp.concatenate([from_matrix(high), from_matrix(total - high)], axis=0)
    owned_all = mm(both_parts, parts)
    parity = place_ref[2]
    half = own_count // 2
    for s in range(pair_count):
        owned = owned_all[s * own_count : (s + 1) * own_count]
        first, second = owned[:half], owned[half:]
        keep = jnp.where(parity == 0, first, second)
        send = jnp.where(parity == 0, second, first)
        for q in range(NQ):
            keep_ref[s, q * half : (q + 1) * half, :] = keep[:, q * LANE : (q + 1) * LANE]
            send_ref[s, q * half : (q + 1) * half, :] = send[:, q * LANE : (q + 1) * LANE]

    chi = chi * chi_scale
    share = (2 * REACH + 1) * BLK // pair_count
    column = iota((LANE, 1), 0)
    target = block + jnp.maximum(REACH - div(column, BLK), 0)
    at_pair = jnp.zeros((LANE, 1), jnp.int32)
    for s in range(1, pair_count):
        at_pair = at_pair + (column >= s * share).astype(jnp.int32)
    place = mod(at_pair - pair_at + pair_count, pair_count) + (
        ((target & 1) ^ place_ref[2]) * pair_count
    )
    spot = place * lanes + div(target, 2) * share + column - at_pair * share
    spread = onehot(iota((LANE, 2 * pair_count * lanes), 1) == spot)
    placed = mm_split(chi, spread)
    for s in range(pair_count):
        for i in range(lanes // LANE):
            at = slice(NQ * half + i * BLK, NQ * half + (i + 1) * BLK)
            begin = s * lanes + i * LANE
            keep_ref[s, at, :] = placed[:, begin : begin + LANE]
            begin += pair_count * lanes
            send_ref[s, at, :] = placed[:, begin : begin + LANE]


def last_kernel(place_ref, own_ref, other_ref, chi_ref, energy_ref):
    half = energy_ref.shape[0] // 2
    share = chi_ref.shape[1]
    parity = place_ref[2]
    own, other = own_ref[...], other_ref[...]
    first = jnp.where(parity == 0, own, other)
    second = jnp.where(parity == 0, other, own)
    for q in range(NQ):
        at = slice(q * LANE, (q + 1) * LANE)
        energy_ref[:half, at] = first[q * half : (q + 1) * half]
        energy_ref[half:, at] = second[q * half : (q + 1) * half]
    start = (place_ref[0] >> 1) * share
    total = None
    for i in range((own.shape[0] - NQ * half) // BLK):
        at = slice(NQ * half + i * BLK, NQ * half + (i + 1) * BLK)
        chi = jnp.where((place_ref[0] & 1) == parity, own[at], other[at])
        pick = onehot(iota((LANE, LANE), 0) + i * LANE == start + iota((LANE, LANE), 1))
        part = mm_split(chi, pick)
        total = part if total is None else total + part
    chi_ref[...] = total[:, :share]


def call(body, outs, *args, scratch=(), ins=None, flops=10**8):
    full = pl.BlockSpec(memory_space=pltpu.VMEM)
    ins = ins or full
    if ins is not full:
        args = [pltpu.with_memory_space_constraint(a, pltpu.HBM) for a in args]
    return pl.pallas_call(
        body,
        out_shape=outs,
        in_specs=[pl.BlockSpec(memory_space=pltpu.SMEM) if a.ndim == 1 else ins for a in args],
        out_specs=jax.tree.map(lambda o: full, outs),
        scratch_shapes=scratch,
        cost_estimate=pl.CostEstimate(flops=flops, bytes_accessed=10**6, transcendentals=0),
        compiler_params=pltpu.CompilerParams(vmem_limit_bytes=24 << 20),
    )(*args)


def per_device(three_center, tile_live, pair_atoms, green_occ, green_vir, screened):
    block_rows, own_count = three_center.shape[:2]
    aux_count, pair_count = lax.axis_size("aux"), lax.axis_size("pair")
    block, pair_at = lax.axis_index("aux"), lax.axis_index("pair")
    rows = block_rows * own_count
    window = screened.shape[1]
    shape = jax.ShapeDtypeStruct

    def shifted(value, steps, parity=None):
        return lax.ppermute(
            value,
            "aux",
            [
                (s, s + steps)
                for s in range(aux_count)
                if 0 <= s + steps < aux_count and parity in (None, s % 2)
            ],
        )

    def turned(value, steps):
        return lax.ppermute(
            value, "pair", [(s, (s - steps) % pair_count) for s in range(pair_count)]
        )

    def flipped(value, mask):
        return lax.ppermute(value, "aux", [(s, s ^ mask) for s in range(aux_count)])

    far = shifted(three_center, -2)
    near_even = flipped(three_center, 1)
    square = shape((NORB, NORB), BF)

    def part_of(c):
        return shape((CHUNKS[c] * own_count, PAIR), BF)

    def whole_of(c):
        return pltpu.VMEM((CHUNKS[c], own_count, PAIR), BF)

    hbm = pl.BlockSpec(memory_space=pltpu.HBM)
    first_part = call(
        pack_kernel,
        [part_of(0)],
        tile_live,
        three_center,
        scratch=[
            pltpu.VMEM(tile_live.shape, jnp.int32),
            whole_of(0),
            pltpu.SemaphoreType.DMA((2,)),
        ],
        ins=hbm,
    )[0]
    pairs, vir, meta, both, cols, vir_t, second_part = call(
        tables_kernel,
        [
            shape((1, pair_count * own_count), jnp.int32),
            square,
            shape((block_rows, LANE), BF),
            shape((2 * NORB, NORB), BF),
            square,
            square,
            part_of(1),
        ],
        green_occ,
        green_vir,
        screened,
        tile_live,
        pair_atoms.reshape(1, pair_count * own_count),
        three_center,
        scratch=[
            pltpu.VMEM((NORB, NORB), BF),
            pltpu.VMEM(screened.shape, BF),
            pltpu.VMEM(tile_live.shape, jnp.int32),
            whole_of(1),
            pltpu.SemaphoreType.DMA((6,)),
        ],
        ins=hbm,
    )
    parts = [first_part, second_part]
    pieces = []
    for part in parts:
        pieces.append([part] + [turned(part, s) for s in range(1, pair_count)])
    meta_even = flipped(meta, 1)
    meta_far = shifted(meta, -2)
    early = call(
        early_kernel,
        [
            shape((rows, PAIR), F4),
            shape((REACH * rows, rows), BF),
        ],
        meta,
        *parts,
    )
    near_odd = flipped(far, 1)
    meta_odd = flipped(meta_far, 1)
    turn = pair_count == 2
    half_at = (lax.population_count(block) + (pair_at if turn else 0)) & 1
    place = jnp.stack([block, pair_at, half_at]).astype(jnp.int32)

    def joint(value, target):
        return lax.ppermute(
            value,
            ("aux", "pair"),
            [
                (s * pair_count + p, t * pair_count + q)
                for s in range(aux_count)
                for p in range(pair_count)
                for t, q in [target(s, p)]
            ],
        )

    own = []
    for c, count in enumerate(CHUNKS):
        own += call(
            lambda *refs: own_kernel(pair_count, own_count, *refs),
            [
                shape((count, NORB, NORB), BF),
                shape((count, NORB, NORB), BF),
                shape((count * own_count, PAIR), BF),
                shape((count * own_count, PAIR), BF),
            ],
            place,
            pairs,
            *pieces[c],
            both,
            cols,
            vir,
            vir_t,
        )

    lanes = -(-(aux_count // 2) * (window // pair_count) // LANE) * LANE
    message = shape((pair_count, own_count // 2 * NQ + lanes // LANE * BLK, LANE), F4)
    aux_total = block_rows * aux_count
    keep, send = call(
        lambda *refs: window_kernel(
            lanes, 1.0 / math.sqrt(aux_total * NAT * OA * NAT), 1.0 / (OA * NAT), *refs
        ),
        [message, message],
        place,
        pairs,
        meta_even,
        meta_odd,
        meta_far,
        near_even.reshape(rows, PAIR),
        near_odd.reshape(rows, PAIR),
        far.reshape(rows, PAIR),
        cols,
        *early,
        *own,
        *parts,
        scratch=[pltpu.VMEM((rows, PAIR), BF)] * 3,
    )
    total = keep + flipped(send, 1)
    owned = total[0]
    if turn:
        owned = owned + joint(total[1].astype(BF), lambda s, p: (s ^ 1, p ^ 1)).astype(F4)
    else:
        for s in range(1, pair_count):
            owned = owned + turned(total[s].astype(BF), -s).astype(F4)
    masks = [1 << i | 1 for i in range(1, (aux_count - 1).bit_length())]
    for masks_here in zip(masks, masks[1:] + masks[:1]):
        owned = owned + joint(
            owned,
            lambda s, p: (s ^ masks_here[(s.bit_count() + (p if turn else 0)) % 2], p),
        )
    polarizability, self_energy = call(
        last_kernel,
        [
            shape((block_rows, window // pair_count), F4),
            shape((own_count, PAIR), F4),
        ],
        place,
        owned,
        flipped(owned, 1),
    )
    return polarizability, self_energy


def solution(mesh):
    placed = (P("aux", "pair", None), P("aux", "pair"), P(), P(), P(), P("aux", None))
    return jax.shard_map(
        per_device,
        mesh=mesh,
        in_specs=placed,
        out_specs=(P("aux", "pair"), P("pair", None)),
        check_vma=False,
    )
```
